128 devices in a mesh: seq: 16 (over y, x), tensor: 8 (over z, core).
Axes of the slice: x: 4, y: 4, z: 4, core: 2. Of those that a mesh axis runs over, the one named last changes fastest.
Arguments:
- tokens: bfloat16 [8192, 2048], P('seq'), may hold values from -200 to 200
- w_latent: bfloat16 [2048, 512], P(None, 'tensor'), may hold values from -0.125 to 0.125
- w_query: bfloat16 [2048, 2048], P(None, 'tensor'), may hold values from -0.125 to 0.125
- w_key_up: bfloat16 [512, 2048], P(None, 'tensor'), may hold values from -0.25 to 0.25
- w_value_up: bfloat16 [512, 2048], P(None, 'tensor'), may hold values from -0.25 to 0.25
- w_stu_query: bfloat16 [2048, 2048], P(None, 'tensor'), may hold values from -0.125 to 0.125
- w_stu_key: bfloat16 [2048, 2048], P(None, 'tensor'), may hold values from -0.125 to 0.125
- w_stu_value: bfloat16 [2048, 2048], P(None, 'tensor'), may hold values from -0.125 to 0.125
- forget: float32 [8192, 16], P('seq', 'tensor'), may hold values from -1 to 0
Outputs:
- teacher_out: bfloat16 [8192, 2048], P('seq', 'tensor')
- loss_mean: float32 [], replicated
- weight_grad: float32 [2048, 2048], P('seq', 'tensor')
The draws below stay inside these ranges and needn't reach their ends.
All inputs are finite; a program needn't handle non-finite values.
Results may differ from the reference program's by a relative error of at most 0.02.
The reference program's roundings to bfloat16 on the way (of `latent`, `queries`, `weights` and `value_grad`) count: a program that leaves them out, or rounds other values in their place, can miss the bound.
Values may be sent and summed in bfloat16 or wider, within the bound.
A program may use at most 64 MiB of HBM per device.

```python
import math
import jax
import jax.numpy as jnp
from jax import lax

D = 2048
HEAD_COUNT = 16
DH = 128
LAT = 512
TOK_DEV = 512
TOKEN_COUNT = 8192


def draw_tokens(key, part):
    base = jax.random.truncated_normal(jax.random.fold_in(key, 11), -6.0, 6.0, (TOKEN_COUNT, D), jnp.float32)
    return base.astype(jnp.bfloat16)


def draw_forget(key, part):
    keep_share = 0.5
    slow_heads = jax.random.uniform(jax.random.fold_in(key, 21), (1, HEAD_COUNT), jnp.float32) < keep_share
    slow_rate = jnp.exp(jax.random.uniform(jax.random.fold_in(key, 22), (1, HEAD_COUNT), jnp.float32, math.log(0.03), math.log(0.15))) / TOKEN_COUNT
    fast_rate = jnp.exp(jax.random.uniform(jax.random.fold_in(key, 23), (1, HEAD_COUNT), jnp.float32, math.log(1.0 / 50.0), math.log(1.0 / 30.0)))
    head_decay_rate = jnp.where(slow_heads, slow_rate, fast_rate)
    random_perturbation = jnp.exp(jax.random.uniform(jax.random.fold_in(key, 24), (TOKEN_COUNT, HEAD_COUNT), jnp.float32, math.log(0.5), math.log(2.0)))
    block_scale = jnp.exp(jax.random.uniform(jax.random.fold_in(key, 25), (TOKEN_COUNT // TOK_DEV, HEAD_COUNT), jnp.float32, math.log(0.5), math.log(2.0)))
    block_multiplier = jnp.repeat(block_scale, TOK_DEV, axis=0)
    episodes = jax.random.uniform(jax.random.fold_in(key, 26), (TOKEN_COUNT, 1), jnp.float32) < 3.0 / TOKEN_COUNT
    episode_loss = jnp.log(jax.random.uniform(jax.random.fold_in(key, 27), (TOKEN_COUNT, HEAD_COUNT), jnp.float32, 0.5, 0.8))
    return -(head_decay_rate * random_perturbation * block_multiplier) + jnp.where(episodes, episode_loss, 0.0)


def shard_levels(own_key, dims, split, least, largest):
    factor_of, own = 1.0, jax.random.fold_in(own_key, 6)
    for axis_at, parts in split:
        steps = jnp.exp(jax.random.uniform(jax.random.fold_in(own, axis_at), (parts,), jnp.float32, least / len(split), largest / len(split)))
        factor_of = factor_of * jnp.repeat(steps, dims[axis_at] // parts).reshape([-1 if axis == axis_at else 1 for axis in range(len(dims))])
    return factor_of


def normal_values(rng, dims, spread, bound, pieces=(), held_as=jnp.bfloat16):
    entries = spread * jax.random.normal(rng, dims, jnp.float32)
    if pieces:
        entries = entries * shard_levels(rng, dims, pieces, -0.22, 0.18)
    return jnp.clip(entries, -bound, bound).astype(held_as)


def setup_inputs(seed: int = 0) -> dict:
    seeds = jax.random.split(jax.random.key(seed), 10)
    tokens = draw_tokens(jax.random.fold_in(seeds[9], 71), 0)
    w_latent = normal_values(seeds[1], (D, LAT), D ** -0.5, 0.125, ((1, 8),))
    w_query = normal_values(seeds[2], (D, HEAD_COUNT * DH), D ** -0.5, 0.125, ((1, 8),))
    w_key_up = normal_values(seeds[3], (LAT, HEAD_COUNT * DH), LAT ** -0.5, 0.25, ((1, 8),))
    w_value_up = normal_values(seeds[4], (LAT, HEAD_COUNT * DH), LAT ** -0.5, 0.25, ((1, 8),))
    w_stu_query = normal_values(seeds[5], (D, HEAD_COUNT * DH), D ** -0.5, 0.125, ((1, 8),))
    w_stu_key = normal_values(seeds[6], (D, HEAD_COUNT * DH), D ** -0.5, 0.125, ((1, 8),))
    w_stu_value = normal_values(seeds[7], (D, HEAD_COUNT * DH), D ** -0.5, 0.125, ((1, 8),))
    forget = draw_forget(jax.random.fold_in(seeds[9], 71), 0)
    return {"tokens": tokens, "w_latent": w_latent, "w_query": w_query, "w_key_up": w_key_up, "w_value_up": w_value_up, "w_stu_query": w_stu_query, "w_stu_key": w_stu_key, "w_stu_value": w_stu_value, "forget": forget}


NEG_FILL = -1e+30
EPSILON = 1e-06

def split_heads(matrix):
    return matrix.reshape(matrix.shape[0], HEAD_COUNT, DH)

def unit_rows(matrix):
    return matrix * lax.rsqrt(lax.optimization_barrier(jnp.sum(matrix * matrix, axis=-1, keepdims=True)) + EPSILON)

def reference(tokens, w_latent, w_query, w_key_up, w_value_up, w_stu_query, w_stu_key, w_stu_value, forget):
    highest = lax.Precision.HIGHEST
    latent = jnp.dot(tokens, w_latent, preferred_element_type=jnp.float32).astype(jnp.bfloat16)
    queries = jnp.dot(tokens, w_query, preferred_element_type=jnp.float32).astype(jnp.bfloat16)
    keys = jnp.dot(latent, w_key_up, preferred_element_type=jnp.float32).astype(jnp.bfloat16)
    values = jnp.dot(latent, w_value_up, preferred_element_type=jnp.float32).astype(jnp.bfloat16)
    query_all = split_heads(queries.astype(jnp.float32))
    key_all = split_heads(keys.astype(jnp.float32))
    value_all = split_heads(values.astype(jnp.float32))
    block_size = math.gcd(TOKEN_COUNT, 512)
    block_count = TOKEN_COUNT // block_size
    score_scale = 1.0 / math.sqrt(DH)
    every_pos = jnp.arange(TOKEN_COUNT, dtype=jnp.int32)
    block_ids = jnp.arange(block_count, dtype=jnp.int32)

    def teacher_block(block_index):
        first_row = (block_index * block_size).astype(jnp.int32)
        query_part = lax.dynamic_slice_in_dim(query_all, first_row, block_size, 0)
        scores = jnp.einsum('qhd,khd->hqk', query_part, key_all) * score_scale
        positions = first_row + jnp.arange(block_size, dtype=jnp.int32)
        allowed = every_pos[None, :] <= positions[:, None]
        scores = jnp.where(allowed[None], scores, NEG_FILL)
        row_top = lax.optimization_barrier(jnp.max(scores, axis=2, keepdims=True))
        expos = jnp.where(allowed[None], jnp.exp(scores - row_top), 0.0)
        row_total = lax.optimization_barrier(jnp.sum(expos, axis=2))
        weights = expos.astype(jnp.bfloat16).astype(jnp.float32)
        mixed = jnp.einsum('hqk,khd->qhd', weights, value_all) / row_total.T[:, :, None]
        return mixed.reshape(block_size, HEAD_COUNT * DH).astype(jnp.bfloat16)
    teacher_out = lax.map(teacher_block, block_ids).reshape(TOKEN_COUNT, HEAD_COUNT * DH)
    stu_query = unit_rows(split_heads(jnp.dot(tokens, w_stu_query, preferred_element_type=jnp.float32)))
    stu_key = unit_rows(split_heads(jnp.dot(tokens, w_stu_key, preferred_element_type=jnp.float32)))
    stu_value = split_heads(jnp.dot(tokens, w_stu_value, preferred_element_type=jnp.float32))
    cumul = jnp.cumsum(forget, axis=0)

    def student_block(block_index):
        first_row = (block_index * block_size).astype(jnp.int32)
        query_part = lax.dynamic_slice_in_dim(stu_query, first_row, block_size, 0)
        cumul_part = lax.dynamic_slice_in_dim(cumul, first_row, block_size, 0)
        positions = first_row + jnp.arange(block_size, dtype=jnp.int32)
        allowed = every_pos[None, :] <= positions[:, None]
        scores = jnp.einsum('qhd,khd->hqk', query_part, stu_key, precision=highest)
        log_gap = cumul_part.T[:, :, None] - cumul.T[:, None, :]
        decays = jnp.exp(jnp.where(allowed[None], log_gap, NEG_FILL))
        return jnp.einsum('hqk,khd->qhd', scores * decays, stu_value, precision=highest)
    student_out = lax.map(student_block, block_ids).reshape(TOKEN_COUNT, HEAD_COUNT, DH)
    mismatch = student_out - split_heads(teacher_out.astype(jnp.float32))
    loss_mean = jnp.sum(mismatch * mismatch) / (2.0 * TOKEN_COUNT * HEAD_COUNT * DH)
    grad_out = mismatch / math.sqrt(TOKEN_COUNT)

    def value_block(block_index):
        first_row = (block_index * block_size).astype(jnp.int32)
        key_part = lax.dynamic_slice_in_dim(stu_key, first_row, block_size, 0)
        cumul_part = lax.dynamic_slice_in_dim(cumul, first_row, block_size, 0)
        positions = first_row + jnp.arange(block_size, dtype=jnp.int32)
        allowed = positions[:, None] <= every_pos[None, :]
        scores = jnp.einsum('khd,qhd->hkq', key_part, stu_query, precision=highest)
        log_gap = cumul.T[:, None, :] - cumul_part.T[:, :, None]
        decays = jnp.exp(jnp.where(allowed[None], log_gap, NEG_FILL))
        return jnp.einsum('hkq,qhd->khd', scores * decays, grad_out, precision=highest)
    value_grad = lax.map(value_block, block_ids).reshape(TOKEN_COUNT, HEAD_COUNT * DH).astype(jnp.bfloat16)
    weight_grad = jnp.dot(tokens.T, value_grad, preferred_element_type=jnp.float32)
    return (teacher_out, loss_mean, weight_grad)
```

```python
import math

import jax
import jax.numpy as jnp
from jax import lax
from jax.experimental import pallas as pl
from jax.experimental.pallas import tpu as pltpu
from jax.sharding import PartitionSpec as P

F32 = jnp.float32
BF16 = jnp.bfloat16
MESH = pl.DeviceIdType.MESH
NEG_FILL = -1e30
EPSILON = 1e-06

T = 512
D = 2048
HD = 128
NH = 2
W = NH * HD
LAT = 512
HALF = T // 2
ALL_TOKENS = 8192
ALL_HEADS = 16
EXP2_SCALE = math.log2(math.e) / math.sqrt(HD)

AWAY = (
    (0, -1), (-1, 0), (0, 1), (1, 0),
    (0, 2), (2, 0), (-1, -1), (1, -1), (-1, 1), (1, 1),
    (-1, 2), (1, 2), (2, -1), (2, 1),
    (2, 2),
)
LEVEL_AT = (0, 4, 10, 14)


def nt(a, b):
    return lax.dot_general(a, b, (((1,), (1,)), ((), ())), preferred_element_type=F32)


def nn(a, b):
    return jnp.dot(a, b, preferred_element_type=F32)


def tn(a, b):
    return lax.dot_general(a, b, (((0,), (0,)), ((), ())), preferred_element_type=F32)


def pick(index, values):
    out = jnp.int32(values[0])
    for k in range(1, len(values)):
        out = jnp.where(index == k, jnp.int32(values[k]), out)
    return out


def three_parts(a):
    hi = a.astype(BF16)
    rest = a - hi.astype(F32)
    mid = rest.astype(BF16)
    low = (rest - mid.astype(F32)).astype(BF16)
    return hi, mid, low


def kernel(
    tok_h, wl_h, wq_h, wku_h, wvu_h, wsq_h, wsk_h, wsv_h, fg_h,
    tout_ref, loss_ref, wg_ref,
    tok, tokt, wl, wall, wkv, fgv,
    lat, myp, pairin, pairbuf, kbuf, vbuf, qbuf, acc, mrun,
    sq, sk, sv, ccol, crow, mix, sout, startq, endk, vg,
    sx, sy, mx, my, bx, by, lx, ly, lz, lc,
    pw, r1in, r1own, r2in,
    load_sem, pair_s, pair_r, z_s, z_r, gs, gr, ds_, dr,
    st_s, st_r, rs_s, rs_r, ls_s, ls_r,
):
    s = lax.axis_index("seq")
    t = lax.axis_index("tensor")
    y, x = s // 4, s % 4
    z, c = t // 2, t % 2
    hb = c * HALF

    def plane(yy, xx):
        return (yy * 4 + xx, t)

    def x_peer(d):
        return plane(y, (x + d) % 4)

    def y_peer(d):
        return plane((y + d) % 4, x)

    def z_peer(d):
        return (s, ((z + d) % 4) * 2 + c)

    partner = (s, z * 2 + (1 - c))

    def remote(src, dst, send, recv, to):
        return pltpu.make_async_remote_copy(
            src_ref=src, dst_ref=dst, send_sem=send, recv_sem=recv, device_id=to, device_id_type=MESH
        )

    wl[...] = jnp.zeros_like(wl)
    loads = [
        pltpu.make_async_copy(wl_h, wl.at[pl.ds(pl.multiple_of(c * 64, 64), 64), :], load_sem.at[0]),
        pltpu.make_async_copy(tok_h, tok, load_sem.at[1]),
        pltpu.make_async_copy(wq_h, wall.at[0], load_sem.at[2]),
        pltpu.make_async_copy(wsk_h, wall.at[1], load_sem.at[3]),
        pltpu.make_async_copy(wsv_h, wall.at[2], load_sem.at[4]),
        pltpu.make_async_copy(wsq_h, wall.at[3], load_sem.at[5]),
        pltpu.make_async_copy(fg_h, fgv, load_sem.at[6]),
        pltpu.make_async_copy(wku_h, wkv.at[:, 0:W], load_sem.at[7]),
        pltpu.make_async_copy(wvu_h, wkv.at[:, W : 2 * W], load_sem.at[8]),
    ]
    for copy in loads:
        copy.start()
    barrier = pltpu.get_barrier_semaphore()
    peers = [x_peer(d) for d in (1, 2, 3)] + [y_peer(d) for d in (1, 2, 3)]
    peers += [z_peer(d) for d in (1, 2, 3)] + [partner]
    for peer in peers:
        pl.semaphore_signal(barrier, inc=1, device_id=peer, device_id_type=MESH)

    loads[0].wait()
    loads[1].wait()
    myp[...] = nt(tok[...], wl[...]).astype(BF16)
    pl.semaphore_wait(barrier, 10)
    other = pl.multiple_of((1 - c) * HALF, HALF)
    own = pl.multiple_of(hb, HALF)
    to_pair = remote(myp.at[pl.ds(other, HALF), :], pairin, pair_s, pair_r, partner)
    to_pair.start()

    def project(i):
        return nn(tok[...], wall[i])

    loads[2].wait()
    qbuf[...] = project(0).astype(BF16)
    to_pair.wait_recv()
    pairbuf[...] = myp[pl.ds(own, HALF), :] + pairin[...]
    my_slice = lat.at[y, x, z, pl.ds(own, HALF), :]
    to_z = [remote(pairbuf, my_slice, z_s.at[d - 1], z_r.at[d - 1], z_peer(d)) for d in (1, 2, 3)]
    for copy in to_z:
        copy.start()
    lat[y, x, z, pl.ds(own, HALF), :] = pairbuf[...]

    def unit(h, m):
        part = m[:, h * HD : (h + 1) * HD]
        return part * lax.rsqrt(jnp.sum(part * part, axis=-1, keepdims=True) + EPSILON)

    loads[6].wait()
    row_at = lax.broadcasted_iota(jnp.int32, (T, T), 0)
    col_at = lax.broadcasted_iota(jnp.int32, (T, T), 1)
    lower = (col_at <= row_at).astype(BF16)
    f_parts = three_parts(fgv[...])
    crow[0:NH, :] = sum(nt(part, lower) for part in f_parts)
    for h in range(NH):
        spread = [jnp.broadcast_to(part[h : h + 1, :], (HD, T)) for part in f_parts]
        ccol[h] = sum(nt(lower, part) for part in spread)

    loads[3].wait()
    keys_f = project(1)
    loads[4].wait()
    sv[...] = project(2).astype(BF16)
    ends = []
    for h in range(NH):
        cols = slice(h * HD, (h + 1) * HD)
        unit_k = unit(h, keys_f)
        sk[:, cols] = unit_k.astype(BF16)
        end_row = ccol[h, T - 1 : T, :]
        endk[:, cols] = (unit_k * jnp.exp(end_row - ccol[h])).astype(BF16)
        ends.append(end_row)
    blank = jnp.zeros((8 - NH, HD), F32)
    mx[x] = jnp.concatenate(ends + [blank], axis=0)
    for h in range(NH):
        cols = slice(h * HD, (h + 1) * HD)
        sx[x, cols, :] = tn(endk[:, cols], sv[:, cols]).astype(BF16)

    def row_sends(buf, sems, first, peer_of, slot):
        return [
            remote(buf.at[slot], buf.at[slot], sems[0].at[first + d - 1], sems[1].at[first + d - 1], peer_of(d))
            for d in (1, 2, 3)
        ]

    st = (st_s, st_r)
    fwd_x = row_sends(sx, st, 0, x_peer, x) + row_sends(mx, st, 3, x_peer, x)
    for copy in fwd_x:
        copy.start()

    loads[5].wait()
    queries_f = project(3)
    for h in range(NH):
        cols = slice(h * HD, (h + 1) * HD)
        unit_q = unit(h, queries_f)
        sq[:, cols] = unit_q.astype(BF16)
        startq[:, cols] = (unit_q * jnp.exp(ccol[h])).astype(BF16)

    def piece(idx, yy, xx, lo, size, to):
        ref = lat.at[yy % 4, xx % 4, :, pl.ds(pl.multiple_of(hb + lo, 64), size), :]
        return remote(ref, ref, gs.at[idx], gr.at[idx], to)

    xp, xm, yp, ym = x_peer(1), x_peer(3), y_peer(1), y_peer(3)
    level_1 = [
        piece(0, y, x, 0, HALF, xp),
        piece(1, y, x, 0, HALF, xm),
        piece(2, y, x, 0, HALF, yp),
        piece(3, y, x, 0, HALF, ym),
    ]
    level_2 = [
        piece(4, y, x - 1, 0, 128, xp),
        piece(5, y, x + 1, 128, 128, xm),
        piece(6, y - 1, x, 0, 128, yp),
        piece(7, y + 1, x, 128, 128, ym),
        piece(8, y, x - 1, 0, 128, yp),
        piece(9, y, x - 1, 0, 128, ym),
        piece(10, y, x + 1, 0, 128, yp),
        piece(11, y, x + 1, 0, 128, ym),
        piece(12, y - 1, x, 128, 128, xp),
        piece(13, y - 1, x, 128, 128, xm),
        piece(14, y + 1, x, 128, 128, xp),
        piece(15, y + 1, x, 128, 128, xm),
    ]
    level_3 = [
        piece(16, y, x + 2, 0, 128, yp),
        piece(17, y, x + 2, 0, 128, ym),
        piece(18, y + 2, x, 128, 128, xp),
        piece(19, y + 2, x, 128, 128, xm),
        piece(20, y - 1, x - 1, 0, 64, yp),
        piece(21, y + 1, x - 1, 64, 64, ym),
        piece(22, y - 1, x + 1, 0, 64, yp),
        piece(23, y + 1, x + 1, 64, 64, ym),
        piece(24, y - 1, x - 1, 128, 64, xp),
        piece(25, y - 1, x + 1, 192, 64, xm),
        piece(26, y + 1, x - 1, 128, 64, xp),
        piece(27, y + 1, x + 1, 192, 64, xm),
    ]
    level_4 = [
        piece(28, y - 1, x + 2, 0, 64, yp),
        piece(29, y + 1, x + 2, 64, 64, ym),
        piece(30, y + 2, x - 1, 128, 64, xp),
        piece(31, y + 2, x + 1, 192, 64, xm),
    ]
    levels = (level_1, level_2, level_3, level_4)

    def to_partner(i, yy, xx):
        ref = lat.at[yy, xx, :, pl.ds(own, HALF), :]
        return remote(ref, ref, ds_.at[i], dr.at[i], partner)

    def away(i):
        return (y + AWAY[i][0]) % 4, (x + AWAY[i][1]) % 4

    for copy in to_z:
        copy.wait_recv()
    for copy in level_1:
        copy.start()
    own_to_partner = to_partner(15, y, x)
    own_to_partner.start()

    for h in range(NH):
        cols = slice(h * HD, (h + 1) * HD)
        raw = nt(sq[:, cols], sk[:, cols])
        gaps = ccol[h, :, 0:1] - crow[h : h + 1, :]
        mix[h] = (raw * jnp.exp(jnp.where(col_at <= row_at, gaps, NEG_FILL))).astype(BF16)
    for h in range(NH):
        cols = slice(h * HD, (h + 1) * HD)
        sout[:, cols] = nn(mix[h], sv[:, cols])

    for copy in fwd_x:
        copy.wait_recv()

    def stage(buf, decays, position, order, h):
        rows = slice(h * HD, (h + 1) * HD)
        running = jnp.zeros((HD, HD), F32)
        total = jnp.zeros((1, HD), F32)
        inside, inside_log = running, total
        for k in order:
            here = position == k
            inside = jnp.where(here, running, inside)
            inside_log = jnp.where(here, total, inside_log)
            log_decay = decays[k, h : h + 1, :]
            running = running * jnp.exp(log_decay) + buf[k, rows, :].astype(F32)
            total = total + log_decay
        return inside, inside_log, running, total

    rise, fall = (0, 1, 2, 3), (3, 2, 1, 0)
    row_inside, ends = [], []
    for h in range(NH):
        inside, inside_log, running, total = stage(sx, mx, x, rise, h)
        row_inside.append((inside, inside_log))
        sy[y, h * HD : (h + 1) * HD, :] = running.astype(BF16)
        ends.append(total)
    my[y] = jnp.concatenate(ends + [blank], axis=0)
    fwd_y = row_sends(sy, st, 6, y_peer, y) + row_sends(my, st, 9, y_peer, y)
    for copy in fwd_y:
        copy.start()

    def tok_turn(i, carry):
        cut = pl.ds(pl.multiple_of(i * 256, 256), 256)
        tokt[cut, :] = jnp.transpose(tok[:, cut])
        return carry

    lax.fori_loop(0, D // 256, tok_turn, 0)

    for h in range(NH):
        vbuf[h, :, HD:W] = jnp.ones((T, HD), BF16)
    loads[7].wait()
    loads[8].wait()

    def up(yy, xx):
        block = jnp.concatenate([lat[yy, xx, k] for k in range(4)], axis=1)
        kbuf[...] = nn(block, wkv[:, 0:W]).astype(BF16)
        values = nn(block, wkv[:, W : 2 * W]).astype(BF16)
        for h in range(NH):
            vbuf[h, :, 0:HD] = values[:, h * HD : (h + 1) * HD]

    own_to_partner.wait_recv()
    up(y, x)
    for h in range(NH):
        cols = slice(h * HD, (h + 1) * HD)
        for part in range(4):
            rows = slice(part * 128, (part + 1) * 128)
            upto = (part + 1) * 128
            scores = nt(qbuf[rows, cols], kbuf[0:upto, cols])
            r = lax.broadcasted_iota(jnp.int32, (128, upto), 0) + part * 128
            k = lax.broadcasted_iota(jnp.int32, (128, upto), 1)
            scores = jnp.where(k <= r, scores, NEG_FILL)
            best = jnp.max(scores, axis=1, keepdims=True)
            weights = jnp.exp2((scores - best) * EXP2_SCALE).astype(BF16)
            acc[h, rows, :] = nn(weights, vbuf[h, 0:upto, :])
            mrun[h, rows, :] = jnp.broadcast_to(best, (128, HD))

    def block_step(i, carry):
        for n, first in enumerate(LEVEL_AT):

            @pl.when(i == first)
            def _():
                for copy in levels[n]:
                    copy.wait_recv()
                if n < 3:
                    for copy in levels[n + 1]:
                        copy.start()
                last = LEVEL_AT[n + 1] if n < 3 else 15
                for b in range(first, last):
                    to_partner(b, *away(b)).start()

        yy = (y + pick(i, [a[0] for a in AWAY]) + 4) % 4
        xx = (x + pick(i, [a[1] for a in AWAY]) + 4) % 4
        to_partner(i, yy, xx).wait_recv()

        @pl.when(yy * 4 + xx < s)
        def _():
            up(yy, xx)
            for h in range(NH):
                cols = slice(h * HD, (h + 1) * HD)
                for part in range(4):
                    rows = slice(part * 128, (part + 1) * 128)
                    scores = nt(qbuf[rows, cols], kbuf[:, cols])
                    old = mrun[h, rows, :]
                    best = jnp.maximum(old, jnp.max(scores, axis=1, keepdims=True))
                    weights = jnp.exp2((scores - best[:, 0:1]) * EXP2_SCALE).astype(BF16)
                    factor = jnp.exp2((old - best) * EXP2_SCALE)
                    both = jnp.concatenate([factor, factor], axis=1)
                    acc[h, rows, :] = acc[h, rows, :] * both + nn(weights, vbuf[h])
                    mrun[h, rows, :] = best

        return carry

    lax.fori_loop(0, 15, block_step, 0)

    for copy in fwd_y:
        copy.wait_recv()
    for h in range(NH):
        cols = slice(h * HD, (h + 1) * HD)
        inside_y = stage(sy, my, y, rise, h)[0]
        inside, inside_log = row_inside[h]
        prefix = (inside + jnp.exp(inside_log) * inside_y).astype(BF16)
        sout[:, cols] = sout[:, cols] + nn(startq[:, cols], prefix)

    squares = jnp.zeros((8, HD), F32)
    inv = 1.0 / math.sqrt(ALL_TOKENS)
    for h in range(NH):
        cols = slice(h * HD, (h + 1) * HD)
        teacher = (acc[h, :, 0:HD] / acc[h, :, HD:W]).astype(BF16)
        tout_ref[:, cols] = teacher
        mismatch = sout[:, cols] - teacher.astype(F32)
        squares += jnp.sum((mismatch * mismatch).reshape(T // 8, 8, HD), axis=0)
        vg[:, cols] = (mismatch * inv).astype(BF16)
    for h in range(NH):
        cols = slice(h * HD, (h + 1) * HD)
        bx[x, cols, :] = tn(startq[:, cols], vg[:, cols]).astype(BF16)
    lx[x] = squares
    ls = (ls_s, ls_r)
    back_x = row_sends(bx, st, 12, x_peer, x)
    loss_x = row_sends(lx, ls, 0, x_peer, x)
    for copy in back_x + loss_x:
        copy.start()
    for h in range(NH):
        cols = slice(h * HD, (h + 1) * HD)
        sout[:, cols] = tn(mix[h], vg[:, cols])

    for copy in back_x:
        copy.wait_recv()
    row_inside = []
    for h in range(NH):
        inside, inside_log, running, _ = stage(bx, mx, x, fall, h)
        row_inside.append((inside, inside_log))
        by[y, h * HD : (h + 1) * HD, :] = running.astype(BF16)
    back_y = row_sends(by, st, 15, y_peer, y)
    for copy in back_y:
        copy.start()
    for copy in loss_x:
        copy.wait_recv()
    ly[y] = lx[0] + lx[1] + lx[2] + lx[3]
    loss_y = row_sends(ly, ls, 3, y_peer, y)
    for copy in loss_y:
        copy.start()
    for copy in back_y:
        copy.wait_recv()
    for h in range(NH):
        cols = slice(h * HD, (h + 1) * HD)
        inside_y = stage(by, my, y, fall, h)[0]
        inside, inside_log = row_inside[h]
        suffix = (inside + jnp.exp(inside_log) * inside_y).astype(BF16)
        vg[:, cols] = (sout[:, cols] + nn(endk[:, cols], suffix)).astype(BF16)

    def wgrad(i, carry):
        part = nn(tokt[pl.ds(pl.multiple_of(i * 512, 512), 512), :], vg[...]).astype(BF16)
        for k in range(4):
            for h in range(NH):
                pw[h, i, k] = part[k * 128 : (k + 1) * 128, h * HD : (h + 1) * HD]
        return carry

    lax.fori_loop(0, 4, wgrad, 0)
    rs_x1 = [
        remote(pw.at[0, :, (x + d) % 4], r1in.at[0, d - 1], rs_s.at[d - 1], rs_r.at[d - 1], x_peer(d))
        for d in (1, 2, 3)
    ]
    rs_y1 = [
        remote(pw.at[1, (y + d) % 4], r1in.at[1, d - 1], rs_s.at[d + 2], rs_r.at[d + 2], y_peer(d))
        for d in (1, 2, 3)
    ]
    for copy in rs_x1 + rs_y1:
        copy.start()
    for copy in loss_y:
        copy.wait_recv()
    lz[z] = ly[0] + ly[1] + ly[2] + ly[3]
    loss_z = row_sends(lz, ls, 6, z_peer, z)
    for copy in loss_z:
        copy.start()

    for copy in rs_x1:
        copy.wait_recv()
    mine = [pw[0, k, x].astype(F32) for k in range(4)]
    for k in range(4):
        r1own[0, k] = (mine[k] + sum(r1in[0, d, k].astype(F32) for d in range(3))).astype(BF16)
    rs_y2 = [
        remote(r1own.at[0, (y + d) % 4], r2in.at[0, d - 1], rs_s.at[d + 5], rs_r.at[d + 5], y_peer(d))
        for d in (1, 2, 3)
    ]
    for copy in rs_y2:
        copy.start()
    for copy in rs_y1:
        copy.wait_recv()
    mine = [pw[1, y, k].astype(F32) for k in range(4)]
    for k in range(4):
        r1own[1, k] = (mine[k] + sum(r1in[1, d, k].astype(F32) for d in range(3))).astype(BF16)
    rs_x2 = [
        remote(r1own.at[1, (x + d) % 4], r2in.at[1, d - 1], rs_s.at[d + 8], rs_r.at[d + 8], x_peer(d))
        for d in (1, 2, 3)
    ]
    for copy in rs_x2:
        copy.start()

    for copy in loss_z:
        copy.wait_recv()
    lc[c] = lz[0] + lz[1] + lz[2] + lz[3]
    loss_c = remote(lc.at[c], lc.at[c], ls_s.at[9], ls_r.at[9], partner)
    loss_c.start()
    loss_c.wait_recv()
    loss_ref[0, 0] = jnp.sum(lc[0] + lc[1]) / (2.0 * ALL_TOKENS * ALL_HEADS * HD)

    for copy in rs_y2:
        copy.wait_recv()
    wg_ref[:, 0:HD] = r1own[0, y].astype(F32) + sum(r2in[0, d].astype(F32) for d in range(3))
    for copy in rs_x2:
        copy.wait_recv()
    wg_ref[:, HD:W] = r1own[1, x].astype(F32) + sum(r2in[1, d].astype(F32) for d in range(3))

    sent = [to_pair] + to_z + fwd_x + fwd_y + back_x + back_y
    sent += loss_x + loss_y + loss_z + [loss_c] + rs_x1 + rs_y1 + rs_y2 + rs_x2
    for level in levels:
        sent += level
    sent += [to_partner(b, *away(b)) for b in range(15)] + [own_to_partner]
    for copy in sent:
        copy.wait_send()


def per_device(tokens, w_latent, w_query, w_key_up, w_value_up, w_stu_query, w_stu_key, w_stu_value, forget):
    dma = pltpu.SemaphoreType.DMA
    scratch = [
        pltpu.VMEM((T, D), BF16),
        pltpu.VMEM((D, T), BF16),
        pltpu.VMEM((HD, D), BF16),
        pltpu.VMEM((4, D, W), BF16),
        pltpu.VMEM((LAT, 2 * W), BF16),
        pltpu.VMEM((NH, T), F32),
        pltpu.VMEM((4, 4, 4, T, HD), BF16),
        pltpu.VMEM((T, HD), BF16),
        pltpu.VMEM((HALF, HD), BF16),
        pltpu.VMEM((HALF, HD), BF16),
        pltpu.VMEM((T, W), BF16),
        pltpu.VMEM((NH, T, W), BF16),
        pltpu.VMEM((T, W), BF16),
        pltpu.VMEM((NH, T, W), F32),
        pltpu.VMEM((NH, T, HD), F32),
        pltpu.VMEM((T, W), BF16),
        pltpu.VMEM((T, W), BF16),
        pltpu.VMEM((T, W), BF16),
        pltpu.VMEM((NH, T, HD), F32),
        pltpu.VMEM((8, T), F32),
        pltpu.VMEM((NH, T, T), BF16),
        pltpu.VMEM((T, W), F32),
        pltpu.VMEM((T, W), BF16),
        pltpu.VMEM((T, W), BF16),
        pltpu.VMEM((T, W), BF16),
        pltpu.VMEM((4, W, HD), BF16),
        pltpu.VMEM((4, W, HD), BF16),
        pltpu.VMEM((4, 8, HD), F32),
        pltpu.VMEM((4, 8, HD), F32),
        pltpu.VMEM((4, W, HD), BF16),
        pltpu.VMEM((4, W, HD), BF16),
        pltpu.VMEM((4, 8, HD), F32),
        pltpu.VMEM((4, 8, HD), F32),
        pltpu.VMEM((4, 8, HD), F32),
        pltpu.VMEM((2, 8, HD), F32),
        pltpu.VMEM((NH, 4, 4, 128, HD), BF16),
        pltpu.VMEM((NH, 3, 4, 128, HD), BF16),
        pltpu.VMEM((NH, 4, 128, HD), BF16),
        pltpu.VMEM((NH, 3, 128, HD), BF16),
        dma((9,)),
        dma,
        dma,
        dma((3,)),
        dma((3,)),
        dma((32,)),
        dma((32,)),
        dma((16,)),
        dma((16,)),
        dma((18,)),
        dma((18,)),
        dma((12,)),
        dma((12,)),
        dma((10,)),
        dma((10,)),
    ]
    anywhere = pl.BlockSpec(memory_space=pl.ANY)
    teacher, loss, wgrad = pl.pallas_call(
        kernel,
        out_shape=(
            jax.ShapeDtypeStruct((T, W), BF16),
            jax.ShapeDtypeStruct((1, 1), F32),
            jax.ShapeDtypeStruct((128, W), F32),
        ),
        in_specs=[anywhere] * 9,
        out_specs=(
            pl.BlockSpec(memory_space=pltpu.VMEM),
            pl.BlockSpec(memory_space=pltpu.SMEM),
            pl.BlockSpec(memory_space=pltpu.VMEM),
        ),
        scratch_shapes=scratch,
        compiler_params=pltpu.CompilerParams(
            collective_id=0, has_side_effects=True, vmem_limit_bytes=60 * 1024 * 1024
        ),
    )(
        tokens, w_latent.T, w_query, w_key_up, w_value_up, w_stu_query, w_stu_key, w_stu_value, forget.T
    )
    return teacher, loss[0, 0], wgrad


def solution(mesh):
    return jax.shard_map(
        per_device,
        mesh=mesh,
        in_specs=(
            P("seq", None),
            P(None, "tensor"),
            P(None, "tensor"),
            P(None, "tensor"),
            P(None, "tensor"),
            P(None, "tensor"),
            P(None, "tensor"),
            P(None, "tensor"),
            P("seq", "tensor"),
        ),
        out_specs=(P("seq", "tensor"), P(), P("seq", "tensor")),
        check_vma=False,
    )
```

```python
import math

import jax
import jax.numpy as jnp
from jax import lax
from jax.experimental import pallas as pl
from jax.experimental.pallas import tpu as pltpu
from jax.sharding import PartitionSpec as P

F32 = jnp.float32
BF16 = jnp.bfloat16
MESH = pl.DeviceIdType.MESH
NEG_FILL = -1e30
EPSILON = 1e-06

T = 512
D = 2048
HD = 128
NH = 2
W = NH * HD
LAT = 512
HALF = T // 2
ONES = 16
ALL_TOKENS = 8192
ALL_HEADS = 16
EXP2_SCALE = math.log2(math.e) / math.sqrt(HD)

AWAY = (
    (-1, 0), (1, 0), (0, -1), (0, 1),
    (2, 0), (-1, -1), (1, -1), (-1, 1), (1, 1), (0, 2),
    (-1, 2), (1, 2), (2, -1), (2, 1),
    (2, 2),
)
LEVEL_BLOCKS = ((0, 4), (4, 10), (10, 14), (14, 15))
LEVEL_STEP = (None, 0, 2, 3)


def nt(a, b):
    return lax.dot_general(a, b, (((1,), (1,)), ((), ())), preferred_element_type=F32)


def nn(a, b):
    return jnp.dot(a, b, preferred_element_type=F32)


def tn(a, b):
    return lax.dot_general(a, b, (((0,), (0,)), ((), ())), preferred_element_type=F32)


def pick(index, values):
    out = jnp.int32(values[0])
    for k in range(1, len(values)):
        out = jnp.where(index == k, jnp.int32(values[k]), out)
    return out


def three_parts(a):
    hi = a.astype(BF16)
    rest = a - hi.astype(F32)
    mid = rest.astype(BF16)
    low = (rest - mid.astype(F32)).astype(BF16)
    return hi, mid, low


def kernel(
    tok_h, wl_h, wq_h, wku_h, wvu_h, wsq_h, wsk_h, wsv_h, fg_h,
    tout_ref, loss_ref, wg_ref,
    tok, tokt, wl, wall, wk, wv, wvt, fgv,
    lat, myp, pairin, pairbuf, kbuf, vt, qbuf, acc, mrun,
    sq, sk, sv, ccol, crow, mix, sout, startq, endk, vg,
    held, heldlog, sx, sy, mx, my, bx, by, lx, ly, lz, lc,
    pw, r1in, r1own, r2in,
    load_sem, pair_s, pair_r, z_s, z_r, gs, gr, zg_s, zg_r, ds_, dr,
    st_s, st_r, rs_s, rs_r, ls_s, ls_r,
):
    s = lax.axis_index("seq")
    t = lax.axis_index("tensor")
    y, x = s // 4, s % 4
    z, c = t // 2, t % 2
    hb = c * HALF

    def plane(yy, xx):
        return (yy * 4 + xx, t)

    def x_peer(d):
        return plane(y, (x + d) % 4)

    def y_peer(d):
        return plane((y + d) % 4, x)

    def z_peer(d):
        return (s, ((z + d) % 4) * 2 + c)

    partner = (s, z * 2 + (1 - c))

    def remote(src, dst, send, recv, to):
        return pltpu.make_async_remote_copy(
            src_ref=src, dst_ref=dst, send_sem=send, recv_sem=recv, device_id=to, device_id_type=MESH
        )

    wl[...] = jnp.zeros_like(wl)
    loads = [
        pltpu.make_async_copy(wl_h, wl.at[pl.ds(pl.multiple_of(c * 64, 64), 64), :], load_sem.at[0]),
        pltpu.make_async_copy(tok_h, tok, load_sem.at[1]),
        pltpu.make_async_copy(wq_h, wall.at[0], load_sem.at[2]),
        pltpu.make_async_copy(wsk_h, wall.at[1], load_sem.at[3]),
        pltpu.make_async_copy(wsv_h, wall.at[2], load_sem.at[4]),
        pltpu.make_async_copy(wsq_h, wall.at[3], load_sem.at[5]),
        pltpu.make_async_copy(fg_h, fgv, load_sem.at[6]),
    ]
    for j in range(4):
        rows = pl.ds(pl.multiple_of((z + j) % 4 * HD, HD), HD)
        loads.append(pltpu.make_async_copy(wku_h.at[rows, :], wk.at[j * HD : (j + 1) * HD, :], load_sem.at[7 + j]))
        loads.append(pltpu.make_async_copy(wvu_h.at[rows, :], wv.at[j * HD : (j + 1) * HD, :], load_sem.at[11 + j]))
    loads[0].start()
    loads[1].start()
    barrier = pltpu.get_barrier_semaphore()
    peers = [x_peer(d) for d in (1, 2, 3)] + [y_peer(d) for d in (1, 2, 3)]
    peers += [z_peer(d) for d in (1, 2, 3)] + [partner]
    for peer in peers:
        pl.semaphore_signal(barrier, inc=1, device_id=peer, device_id_type=MESH)

    loads[0].wait()
    loads[1].wait()
    for copy in loads[2:]:
        copy.start()
    myp[...] = nt(tok[...], wl[...]).astype(BF16)
    pl.semaphore_wait(barrier, 10)
    other = pl.multiple_of((1 - c) * HALF, HALF)
    own = pl.multiple_of(hb, HALF)
    to_pair = remote(myp.at[pl.ds(other, HALF), :], pairin, pair_s, pair_r, partner)
    to_pair.start()

    def project(i):
        return nn(tok[...], wall[i])

    loads[2].wait()
    qbuf[...] = project(0).astype(BF16)
    to_pair.wait_recv()
    pairbuf[...] = myp[pl.ds(own, HALF), :] + pairin[...]
    my_slice = lat.at[y, x, z, pl.ds(own, HALF), :]
    lat[y, x, 0, pl.ds(own, HALF), :] = pairbuf[...]

    def slot(yy, xx, j):
        return lat.at[yy, xx, j, pl.ds(own, HALF), :]

    to_z = [
        remote(pairbuf, slot(y, x, 4 - d), z_s.at[d - 1], z_r.at[d - 1], z_peer(d)) for d in (1, 2, 3)
    ]
    for d in (3, 1, 2):
        to_z[d - 1].start()
    xp, xm, yp, ym = x_peer(1), x_peer(3), y_peer(1), y_peer(3)

    def near(j):
        return [
            remote(slot(y, x, j), slot(y, x, j), gs.at[32 + 2 * k + j], gr.at[32 + 2 * k + j], to)
            for k, to in enumerate((yp, ym, xp, xm))
        ]

    level_1 = [near(0), near(1)]
    for copy in level_1[0]:
        copy.start()

    def unit(h, m):
        part = m[:, h * HD : (h + 1) * HD]
        return part * lax.rsqrt(jnp.sum(part * part, axis=-1, keepdims=True) + EPSILON)

    loads[6].wait()
    row_at = lax.broadcasted_iota(jnp.int32, (T, T), 0)
    col_at = lax.broadcasted_iota(jnp.int32, (T, T), 1)
    lower = (col_at <= row_at).astype(BF16)
    f_parts = three_parts(fgv[...])
    crow[0:NH, :] = sum(nt(part, lower) for part in f_parts)
    for h in range(NH):
        spread = [jnp.broadcast_to(part[h : h + 1, :], (HD, T)) for part in f_parts]
        ccol[h] = sum(nt(lower, part) for part in spread)

    loads[3].wait()
    keys_f = project(1)
    loads[4].wait()
    sv[...] = project(2).astype(BF16)
    to_z[2].wait_recv()
    for copy in level_1[1]:
        copy.start()
    ends = []
    for h in range(NH):
        cols = slice(h * HD, (h + 1) * HD)
        unit_k = unit(h, keys_f)
        sk[:, cols] = unit_k.astype(BF16)
        end_row = ccol[h, T - 1 : T, :]
        endk[:, cols] = (unit_k * jnp.exp(end_row - ccol[h])).astype(BF16)
        ends.append(end_row)
    blank = jnp.zeros((8 - NH, HD), F32)
    mx[x] = jnp.concatenate(ends + [blank], axis=0)
    for h in range(NH):
        cols = slice(h * HD, (h + 1) * HD)
        sx[x, cols, :] = tn(endk[:, cols], sv[:, cols]).astype(BF16)

    def row_sends(buf, sems, first, peer_of, slot):
        return [
            remote(buf.at[slot], buf.at[slot], sems[0].at[first + d - 1], sems[1].at[first + d - 1], peer_of(d))
            for d in (1, 2, 3)
        ]

    st = (st_s, st_r)
    fwd_x = row_sends(sx, st, 0, x_peer, x) + row_sends(mx, st, 3, x_peer, x)
    loads[5].wait()
    queries_f = project(3)
    for h in range(NH):
        cols = slice(h * HD, (h + 1) * HD)
        unit_q = unit(h, queries_f)
        sq[:, cols] = unit_q.astype(BF16)
        startq[:, cols] = (unit_q * jnp.exp(ccol[h])).astype(BF16)

    def piece(idx, yy, xx, lo, size, to):
        ref = lat.at[yy % 4, xx % 4, 0:2, pl.ds(pl.multiple_of(hb + lo, 64), size), :]
        return remote(ref, ref, gs.at[idx], gr.at[idx], to)

    level_2 = [
        piece(4, y, x - 1, 0, 128, xp),
        piece(5, y, x + 1, 128, 128, xm),
        piece(6, y - 1, x, 0, 128, yp),
        piece(7, y + 1, x, 128, 128, ym),
        piece(8, y, x - 1, 0, 128, yp),
        piece(9, y, x - 1, 0, 128, ym),
        piece(10, y, x + 1, 0, 128, yp),
        piece(11, y, x + 1, 0, 128, ym),
        piece(12, y - 1, x, 128, 128, xp),
        piece(13, y - 1, x, 128, 128, xm),
        piece(14, y + 1, x, 128, 128, xp),
        piece(15, y + 1, x, 128, 128, xm),
    ]
    level_3 = [
        piece(16, y, x + 2, 0, 128, yp),
        piece(17, y, x + 2, 0, 128, ym),
        piece(18, y + 2, x, 128, 128, xp),
        piece(19, y + 2, x, 128, 128, xm),
        piece(20, y - 1, x - 1, 0, 64, yp),
        piece(21, y + 1, x - 1, 64, 64, ym),
        piece(22, y - 1, x + 1, 0, 64, yp),
        piece(23, y + 1, x + 1, 64, 64, ym),
        piece(24, y - 1, x - 1, 128, 64, xp),
        piece(25, y - 1, x + 1, 192, 64, xm),
        piece(26, y + 1, x - 1, 128, 64, xp),
        piece(27, y + 1, x + 1, 192, 64, xm),
    ]
    level_4 = [
        piece(28, y - 1, x + 2, 0, 64, yp),
        piece(29, y + 1, x + 2, 64, 64, ym),
        piece(30, y + 2, x - 1, 128, 64, xp),
        piece(31, y + 2, x + 1, 192, 64, xm),
    ]
    levels = (sum(level_1, []), level_2, level_3, level_4)

    def to_partner(i, yy, xx):
        ref = lat.at[yy, xx, :, pl.ds(own, HALF), :]
        return remote(ref, ref, ds_.at[i], dr.at[i], partner)

    def other_slices(b, yy, xx):
        return (
            remote(slot(yy, xx, 0), slot(yy, xx, 3), zg_s.at[2 * b], zg_r.at[2 * b], z_peer(1)),
            remote(slot(yy, xx, 1), slot(yy, xx, 2), zg_s.at[2 * b + 1], zg_r.at[2 * b + 1], z_peer(3)),
        )

    def arrive(n):
        for copy in levels[n]:
            copy.wait_recv()
        if n < 3:
            for copy in levels[n + 1]:
                copy.start()
        for b in range(*LEVEL_BLOCKS[n]):
            for copy in other_slices(b, *away(b)):
                copy.start()

    def away(i):
        return (y + AWAY[i][0]) % 4, (x + AWAY[i][1]) % 4

    to_z[0].wait_recv()
    to_z[1].wait_recv()
    own_to_partner = to_partner(15, y, x)
    own_to_partner.start()
    arrive(0)

    for h in range(NH):
        cols = slice(h * HD, (h + 1) * HD)
        raw = nt(sq[:, cols], sk[:, cols])
        gaps = ccol[h, :, 0:1] - crow[h : h + 1, :]
        mix[h] = (raw * jnp.exp(jnp.where(col_at <= row_at, gaps, NEG_FILL))).astype(BF16)
    for h in range(NH):
        cols = slice(h * HD, (h + 1) * HD)
        sout[:, cols] = nn(mix[h], sv[:, cols])

    def stage(buf, decays, position, order, h):
        rows = slice(h * HD, (h + 1) * HD)
        running = jnp.zeros((HD, HD), F32)
        total = jnp.zeros((1, HD), F32)
        inside, inside_log = running, total
        for k in order:
            here = position == k
            inside = jnp.where(here, running, inside)
            inside_log = jnp.where(here, total, inside_log)
            log_decay = decays[k, h : h + 1, :]
            running = running * jnp.exp(log_decay) + buf[k, rows, :].astype(F32)
            total = total + log_decay
        return inside, inside_log, running, total

    rise, fall = (0, 1, 2, 3), (3, 2, 1, 0)
    fwd_y = row_sends(sy, st, 6, y_peer, y) + row_sends(my, st, 9, y_peer, y)

    def forward_row():
        for copy in fwd_x:
            copy.wait_recv()
        ends = []
        for h in range(NH):
            rows = slice(h * HD, (h + 1) * HD)
            inside, inside_log, running, total = stage(sx, mx, x, rise, h)
            held[rows, :] = inside
            heldlog[h : h + 1, :] = inside_log
            sy[y, rows, :] = running.astype(BF16)
            ends.append(total)
        my[y] = jnp.concatenate(ends + [blank], axis=0)
        for copy in fwd_y:
            copy.start()

    def tok_turn(i, carry):
        cut = pl.ds(pl.multiple_of(i * 256, 256), 256)
        tokt[cut, :] = jnp.transpose(tok[:, cut])
        return carry

    lax.fori_loop(0, D // 256, tok_turn, 0)

    for copy in loads[7:]:
        copy.wait()
    wvt[...] = jnp.transpose(wv[...])
    for h in range(NH):
        vt[h, HD:, :] = jnp.ones((ONES, 2 * T), BF16)

    def attend(blocks, masked=False):
        keys = T * len(blocks)
        arrays = []
        for n, (yy, xx) in enumerate(blocks):
            block = jnp.concatenate([lat[yy, xx, k] for k in range(4)], axis=1)
            kbuf[n * T : (n + 1) * T, :] = nn(block, wk[...]).astype(BF16)
            arrays.append(block)
        scores = [
            nt(kbuf[0:keys, h * HD : (h + 1) * HD], qbuf[:, h * HD : (h + 1) * HD]) for h in range(NH)
        ]
        for n, block in enumerate(arrays):
            values = nt(wvt[...], block).astype(BF16)
            for h in range(NH):
                vt[h, 0:HD, n * T : (n + 1) * T] = values[h * HD : (h + 1) * HD, :]
        for h in range(NH):
            score = scores[h]
            if masked:
                score = jnp.where(row_at <= col_at, score, NEG_FILL)
            best = jnp.max(score, axis=0, keepdims=True)
            if not masked:
                old = mrun[h : h + 1, :]
                best = jnp.maximum(old, best)
            weights = jnp.exp2((score - best) * EXP2_SCALE).astype(BF16)
            part = nn(vt[h, :, 0:keys], weights)
            if not masked:
                part += acc[h] * jnp.exp2((old - best) * EXP2_SCALE)
            acc[h] = part
            mrun[h : h + 1, :] = best

    own_to_partner.wait_recv()
    attend([(y, x)], masked=True)

    def place(b):
        yy = (y + pick(b, [a[0] for a in AWAY]) + 4) % 4
        xx = (x + pick(b, [a[1] for a in AWAY]) + 4) % 4
        return yy, xx

    def pass_on(b):
        yy, xx = place(b)
        for copy in other_slices(b, yy, xx):
            copy.wait_recv()
        to_partner(b, yy, xx).start()

    pass_on(0)
    pass_on(1)

    def block_step(i, carry):
        for n in (1, 2, 3):

            @pl.when(i == LEVEL_STEP[n])
            def _():
                arrive(n)
                if n == 1:
                    for copy in fwd_x:
                        copy.start()
                if n == 3:
                    forward_row()

        @pl.when(i < 7)
        def _():
            pass_on(2 * i + 2)

        @pl.when(i < 6)
        def _():
            pass_on(2 * i + 3)

        y1, x1 = place(2 * i)
        to_partner(2 * i, y1, x1).wait_recv()
        y2, x2 = place(2 * i + 1)

        @pl.when(i < 7)
        def _():
            to_partner(2 * i + 1, y2, x2).wait_recv()

        need_1 = y1 * 4 + x1 < s
        need_2 = jnp.logical_and(y2 * 4 + x2 < s, i < 7)

        @pl.when(jnp.logical_and(need_1, need_2))
        def _():
            attend([(y1, x1), (y2, x2)])

        @pl.when(need_1 != need_2)
        def _():
            attend([(jnp.where(need_1, y1, y2), jnp.where(need_1, x1, x2))])

        return carry

    lax.fori_loop(0, 8, block_step, 0)

    for copy in fwd_y:
        copy.wait_recv()
    for h in range(NH):
        cols = slice(h * HD, (h + 1) * HD)
        inside_y = stage(sy, my, y, rise, h)[0]
        prefix = (held[cols, :] + jnp.exp(heldlog[h : h + 1, :]) * inside_y).astype(BF16)
        sout[:, cols] = sout[:, cols] + nn(startq[:, cols], prefix)

    squares = jnp.zeros((8, HD), F32)
    inv = 1.0 / math.sqrt(ALL_TOKENS)
    for h in range(NH):
        cols = slice(h * HD, (h + 1) * HD)
        teacher = jnp.transpose(acc[h, 0:HD, :] / acc[h, HD : HD + 1, :]).astype(BF16)
        tout_ref[:, cols] = teacher
        mismatch = sout[:, cols] - teacher.astype(F32)
        squares += jnp.sum((mismatch * mismatch).reshape(T // 8, 8, HD), axis=0)
        vg[:, cols] = (mismatch * inv).astype(BF16)
    for h in range(NH):
        cols = slice(h * HD, (h + 1) * HD)
        bx[x, cols, :] = tn(startq[:, cols], vg[:, cols]).astype(BF16)
    lx[x] = squares
    ls = (ls_s, ls_r)
    back_x = row_sends(bx, st, 12, x_peer, x)
    loss_x = row_sends(lx, ls, 0, x_peer, x)
    for copy in back_x + loss_x:
        copy.start()
    for h in range(NH):
        cols = slice(h * HD, (h + 1) * HD)
        sout[:, cols] = tn(mix[h], vg[:, cols])

    for copy in back_x:
        copy.wait_recv()
    row_inside = []
    for h in range(NH):
        inside, inside_log, running, _ = stage(bx, mx, x, fall, h)
        row_inside.append((inside, inside_log))
        by[y, h * HD : (h + 1) * HD, :] = running.astype(BF16)
    back_y = row_sends(by, st, 15, y_peer, y)
    for copy in back_y:
        copy.start()
    for copy in loss_x:
        copy.wait_recv()
    ly[y] = lx[0] + lx[1] + lx[2] + lx[3]
    loss_y = row_sends(ly, ls, 3, y_peer, y)
    for copy in loss_y:
        copy.start()
    for copy in back_y:
        copy.wait_recv()
    for h in range(NH):
        cols = slice(h * HD, (h + 1) * HD)
        inside_y = stage(by, my, y, fall, h)[0]
        inside, inside_log = row_inside[h]
        suffix = (inside + jnp.exp(inside_log) * inside_y).astype(BF16)
        vg[:, cols] = (sout[:, cols] + nn(endk[:, cols], suffix)).astype(BF16)

    def wgrad(i, carry):
        part = nn(tokt[pl.ds(pl.multiple_of(i * 512, 512), 512), :], vg[...]).astype(BF16)
        for k in range(4):
            for h in range(NH):
                pw[h, i, k] = part[k * 128 : (k + 1) * 128, h * HD : (h + 1) * HD]
        return carry

    lax.fori_loop(0, 4, wgrad, 0)
    rs_x1 = [
        remote(pw.at[0, :, (x + d) % 4], r1in.at[0, d - 1], rs_s.at[d - 1], rs_r.at[d - 1], x_peer(d))
        for d in (1, 2, 3)
    ]
    rs_y1 = [
        remote(pw.at[1, (y + d) % 4], r1in.at[1, d - 1], rs_s.at[d + 2], rs_r.at[d + 2], y_peer(d))
        for d in (1, 2, 3)
    ]
    for copy in rs_x1 + rs_y1:
        copy.start()
    for copy in loss_y:
        copy.wait_recv()
    lz[z] = ly[0] + ly[1] + ly[2] + ly[3]
    loss_z = row_sends(lz, ls, 6, z_peer, z)
    for copy in loss_z:
        copy.start()

    for copy in rs_x1:
        copy.wait_recv()
    mine = [pw[0, k, x].astype(F32) for k in range(4)]
    for k in range(4):
        r1own[0, k] = (mine[k] + sum(r1in[0, d, k].astype(F32) for d in range(3))).astype(BF16)
    rs_y2 = [
        remote(r1own.at[0, (y + d) % 4], r2in.at[0, d - 1], rs_s.at[d + 5], rs_r.at[d + 5], y_peer(d))
        for d in (1, 2, 3)
    ]
    for copy in rs_y2:
        copy.start()
    for copy in rs_y1:
        copy.wait_recv()
    mine = [pw[1, y, k].astype(F32) for k in range(4)]
    for k in range(4):
        r1own[1, k] = (mine[k] + sum(r1in[1, d, k].astype(F32) for d in range(3))).astype(BF16)
    rs_x2 = [
        remote(r1own.at[1, (x + d) % 4], r2in.at[1, d - 1], rs_s.at[d + 8], rs_r.at[d + 8], x_peer(d))
        for d in (1, 2, 3)
    ]
    for copy in rs_x2:
        copy.start()

    for copy in loss_z:
        copy.wait_recv()
    lc[c] = lz[0] + lz[1] + lz[2] + lz[3]
    loss_c = remote(lc.at[c], lc.at[c], ls_s.at[9], ls_r.at[9], partner)
    loss_c.start()
    loss_c.wait_recv()
    loss_ref[0, 0] = jnp.sum(lc[0] + lc[1]) / (2.0 * ALL_TOKENS * ALL_HEADS * HD)

    for copy in rs_y2:
        copy.wait_recv()
    wg_ref[:, 0:HD] = r1own[0, y].astype(F32) + sum(r2in[0, d].astype(F32) for d in range(3))
    for copy in rs_x2:
        copy.wait_recv()
    wg_ref[:, HD:W] = r1own[1, x].astype(F32) + sum(r2in[1, d].astype(F32) for d in range(3))

    sent = [to_pair] + to_z + fwd_x + fwd_y + back_x + back_y
    sent += loss_x + loss_y + loss_z + [loss_c] + rs_x1 + rs_y1 + rs_y2 + rs_x2
    for level in levels:
        sent += level
    for b in range(15):
        sent += [*other_slices(b, *away(b)), to_partner(b, *away(b))]
    sent.append(own_to_partner)
    for copy in sent:
        copy.wait_send()


def per_device(tokens, w_latent, w_query, w_key_up, w_value_up, w_stu_query, w_stu_key, w_stu_value, forget):
    dma = pltpu.SemaphoreType.DMA
    scratch = [
        pltpu.VMEM((T, D), BF16),
        pltpu.VMEM((D, T), BF16),
        pltpu.VMEM((HD, D), BF16),
        pltpu.VMEM((4, D, W), BF16),
        pltpu.VMEM((LAT, W), BF16),
        pltpu.VMEM((LAT, W), BF16),
        pltpu.VMEM((W, LAT), BF16),
        pltpu.VMEM((NH, T), F32),
        pltpu.VMEM((4, 4, 4, T, HD), BF16),
        pltpu.VMEM((T, HD), BF16),
        pltpu.VMEM((HALF, HD), BF16),
        pltpu.VMEM((HALF, HD), BF16),
        pltpu.VMEM((2 * T, W), BF16),
        pltpu.VMEM((NH, HD + ONES, 2 * T), BF16),
        pltpu.VMEM((T, W), BF16),
        pltpu.VMEM((NH, HD + ONES, T), F32),
        pltpu.VMEM((8, T), F32),
        pltpu.VMEM((T, W), BF16),
        pltpu.VMEM((T, W), BF16),
        pltpu.VMEM((T, W), BF16),
        pltpu.VMEM((NH, T, HD), F32),
        pltpu.VMEM((8, T), F32),
        pltpu.VMEM((NH, T, T), BF16),
        pltpu.VMEM((T, W), F32),
        pltpu.VMEM((T, W), BF16),
        pltpu.VMEM((T, W), BF16),
        pltpu.VMEM((T, W), BF16),
        pltpu.VMEM((W, HD), F32),
        pltpu.VMEM((8, HD), F32),
        pltpu.VMEM((4, W, HD), BF16),
        pltpu.VMEM((4, W, HD), BF16),
        pltpu.VMEM((4, 8, HD), F32),
        pltpu.VMEM((4, 8, HD), F32),
        pltpu.VMEM((4, W, HD), BF16),
        pltpu.VMEM((4, W, HD), BF16),
        pltpu.VMEM((4, 8, HD), F32),
        pltpu.VMEM((4, 8, HD), F32),
        pltpu.VMEM((4, 8, HD), F32),
        pltpu.VMEM((2, 8, HD), F32),
        pltpu.VMEM((NH, 4, 4, 128, HD), BF16),
        pltpu.VMEM((NH, 3, 4, 128, HD), BF16),
        pltpu.VMEM((NH, 4, 128, HD), BF16),
        pltpu.VMEM((NH, 3, 128, HD), BF16),
        dma((15,)),
        dma,
        dma,
        dma((3,)),
        dma((3,)),
        dma((40,)),
        dma((40,)),
        dma((30,)),
        dma((30,)),
        dma((16,)),
        dma((16,)),
        dma((18,)),
        dma((18,)),
        dma((12,)),
        dma((12,)),
        dma((10,)),
        dma((10,)),
    ]
    anywhere = pl.BlockSpec(memory_space=pl.ANY)
    teacher, loss, wgrad = pl.pallas_call(
        kernel,
        out_shape=(
            jax.ShapeDtypeStruct((T, W), BF16),
            jax.ShapeDtypeStruct((1, 1), F32),
            jax.ShapeDtypeStruct((128, W), F32),
        ),
        in_specs=[anywhere] * 9,
        out_specs=(
            pl.BlockSpec(memory_space=pltpu.VMEM),
            pl.BlockSpec(memory_space=pltpu.SMEM),
            pl.BlockSpec(memory_space=pltpu.VMEM),
        ),
        scratch_shapes=scratch,
        compiler_params=pltpu.CompilerParams(
            collective_id=0, has_side_effects=True, vmem_limit_bytes=60 * 1024 * 1024
        ),
    )(
        tokens, w_latent.T, w_query, w_key_up, w_value_up, w_stu_query, w_stu_key, w_stu_value, forget.T
    )
    return teacher, loss[0, 0], wgrad


def solution(mesh):
    return jax.shard_map(
        per_device,
        mesh=mesh,
        in_specs=(
            P("seq", None),
            P(None, "tensor"),
            P(None, "tensor"),
            P(None, "tensor"),
            P(None, "tensor"),
            P(None, "tensor"),
            P(None, "tensor"),
            P(None, "tensor"),
            P("seq", "tensor"),
        ),
        out_specs=(P("seq", "tensor"), P(), P("seq", "tensor")),
        check_vma=False,
    )
```

```python
import math

import jax
import jax.numpy as jnp
from jax import lax
from jax.experimental import pallas as pl
from jax.experimental.pallas import tpu as pltpu
from jax.sharding import PartitionSpec as P

F32 = jnp.float32
BF16 = jnp.bfloat16
MESH = pl.DeviceIdType.MESH
NEG_FILL = -1e30
EPSILON = 1e-06

T = 512
D = 2048
HD = 128
NH = 2
W = NH * HD
LAT = 512
HALF = T // 2
ONES = 16
ALL_TOKENS = 8192
ALL_HEADS = 16
EXP2_SCALE = math.log2(math.e) / math.sqrt(HD)

AWAY = (
    (-1, 0), (1, 0), (0, -1), (0, 1),
    (-1, -1), (1, -1), (-1, 1), (1, 1),
    (2, 0), (0, 2),
    (-1, 2), (1, 2), (2, -1), (2, 1),
    (2, 2),
)
LEVEL_OVER_Z = ((0, 4), (4, 8), (10, 14), (14, 15))
LEVEL_STEP = (None, 0, 2, 3)


def nt(a, b):
    return lax.dot_general(a, b, (((1,), (1,)), ((), ())), preferred_element_type=F32)


def nn(a, b):
    return jnp.dot(a, b, preferred_element_type=F32)


def tn(a, b):
    return lax.dot_general(a, b, (((0,), (0,)), ((), ())), preferred_element_type=F32)


def pick(index, values):
    out = jnp.int32(values[0])
    for k in range(1, len(values)):
        out = jnp.where(index == k, jnp.int32(values[k]), out)
    return out


def three_parts(a):
    hi = a.astype(BF16)
    rest = a - hi.astype(F32)
    mid = rest.astype(BF16)
    low = (rest - mid.astype(F32)).astype(BF16)
    return hi, mid, low


def kernel(
    tok_h, wl_h, wq_h, wku_h, wvu_h, wsq_h, wsk_h, wsv_h, fg_h,
    tout_ref, loss_ref, wg_ref,
    tok, tokt, wl, wall, wk, wv, wvt, fgv,
    lat, myp, pairin, pairbuf, kbuf, vt, qbuf, acc, mrun,
    sq, sk, sv, ccol, crow, mix, sout, startq, endk, vg,
    held, heldlog, sx, sy, mx, my, bx, by, lx, ly, lz, lc,
    pw, r1in, r1own, r2in,
    load_sem, pair_s, pair_r, z_s, z_r, gs, gr, zg_s, zg_r, ds_, dr,
    st_s, st_r, rs_s, rs_r, ls_s, ls_r,
):
    s = lax.axis_index("seq")
    t = lax.axis_index("tensor")
    y, x = s // 4, s % 4
    z, c = t // 2, t % 2
    hb = c * HALF

    def plane(yy, xx):
        return (yy * 4 + xx, t)

    def x_peer(d):
        return plane(y, (x + d) % 4)

    def y_peer(d):
        return plane((y + d) % 4, x)

    def z_peer(d):
        return (s, ((z + d) % 4) * 2 + c)

    partner = (s, z * 2 + (1 - c))

    def remote(src, dst, send, recv, to):
        return pltpu.make_async_remote_copy(
            src_ref=src, dst_ref=dst, send_sem=send, recv_sem=recv, device_id=to, device_id_type=MESH
        )

    wl[...] = jnp.zeros_like(wl)
    loads = [
        pltpu.make_async_copy(wl_h, wl.at[pl.ds(pl.multiple_of(c * 64, 64), 64), :], load_sem.at[0]),
        pltpu.make_async_copy(tok_h, tok, load_sem.at[1]),
        pltpu.make_async_copy(wq_h, wall.at[0], load_sem.at[2]),
        pltpu.make_async_copy(wsk_h, wall.at[1], load_sem.at[3]),
        pltpu.make_async_copy(wsv_h, wall.at[2], load_sem.at[4]),
        pltpu.make_async_copy(wsq_h, wall.at[3], load_sem.at[5]),
        pltpu.make_async_copy(fg_h, fgv, load_sem.at[6]),
    ]
    for j in range(4):
        rows = pl.ds(pl.multiple_of((z + j) % 4 * HD, HD), HD)
        loads.append(pltpu.make_async_copy(wku_h.at[rows, :], wk.at[j * HD : (j + 1) * HD, :], load_sem.at[7 + j]))
        loads.append(pltpu.make_async_copy(wvu_h.at[rows, :], wv.at[j * HD : (j + 1) * HD, :], load_sem.at[11 + j]))
    loads[0].start()
    loads[1].start()
    barrier = pltpu.get_barrier_semaphore()
    peers = [x_peer(d) for d in (1, 2, 3)] + [y_peer(d) for d in (1, 2, 3)]
    peers += [z_peer(d) for d in (1, 2, 3)] + [partner]
    for peer in peers:
        pl.semaphore_signal(barrier, inc=1, device_id=peer, device_id_type=MESH)

    loads[0].wait()
    loads[1].wait()
    for copy in loads[2:]:
        copy.start()
    myp[...] = nt(tok[...], wl[...]).astype(BF16)
    pl.semaphore_wait(barrier, 10)
    other = pl.multiple_of((1 - c) * HALF, HALF)
    own = pl.multiple_of(hb, HALF)
    to_pair = remote(myp.at[pl.ds(other, HALF), :], pairin, pair_s, pair_r, partner)
    to_pair.start()

    def project(i):
        return nn(tok[...], wall[i])

    loads[2].wait()
    qbuf[...] = project(0).astype(BF16)
    to_pair.wait_recv()
    pairbuf[...] = myp[pl.ds(own, HALF), :] + pairin[...]
    my_slice = lat.at[y, x, z, pl.ds(own, HALF), :]
    lat[y, x, 0, pl.ds(own, HALF), :] = pairbuf[...]

    def slot(yy, xx, j):
        return lat.at[yy, xx, j, pl.ds(own, HALF), :]

    to_z = [
        remote(pairbuf, slot(y, x, 4 - d), z_s.at[d - 1], z_r.at[d - 1], z_peer(d)) for d in (1, 2, 3)
    ]
    for d in (3, 1, 2):
        to_z[d - 1].start()
    xp, xm, yp, ym = x_peer(1), x_peer(3), y_peer(1), y_peer(3)

    def near(j):
        return [
            remote(slot(y, x, j), slot(y, x, j), gs.at[32 + 2 * k + j], gr.at[32 + 2 * k + j], to)
            for k, to in enumerate((yp, ym, xp, xm))
        ]

    level_1 = [near(0), near(1)]
    for copy in level_1[0]:
        copy.start()

    def unit(h, m):
        part = m[:, h * HD : (h + 1) * HD]
        return part * lax.rsqrt(jnp.sum(part * part, axis=-1, keepdims=True) + EPSILON)

    loads[6].wait()
    row_at = lax.broadcasted_iota(jnp.int32, (T, T), 0)
    col_at = lax.broadcasted_iota(jnp.int32, (T, T), 1)
    lower = (col_at <= row_at).astype(BF16)
    f_parts = three_parts(fgv[...])
    crow[0:NH, :] = sum(nt(part, lower) for part in f_parts)
    for h in range(NH):
        spread = [jnp.broadcast_to(part[h : h + 1, :], (HD, T)) for part in f_parts]
        ccol[h] = sum(nt(lower, part) for part in spread)

    loads[3].wait()
    keys_f = project(1)
    loads[4].wait()
    sv[...] = project(2).astype(BF16)
    to_z[2].wait_recv()
    for copy in level_1[1]:
        copy.start()
    ends = []
    for h in range(NH):
        cols = slice(h * HD, (h + 1) * HD)
        unit_k = unit(h, keys_f)
        sk[:, cols] = unit_k.astype(BF16)
        end_row = ccol[h, T - 1 : T, :]
        endk[:, cols] = (unit_k * jnp.exp(end_row - ccol[h])).astype(BF16)
        ends.append(end_row)
    blank = jnp.zeros((8 - NH, HD), F32)
    mx[x] = jnp.concatenate(ends + [blank], axis=0)
    for h in range(NH):
        cols = slice(h * HD, (h + 1) * HD)
        sx[x, cols, :] = tn(endk[:, cols], sv[:, cols]).astype(BF16)

    def row_sends(buf, sems, first, peer_of, slot):
        return [
            remote(buf.at[slot], buf.at[slot], sems[0].at[first + d - 1], sems[1].at[first + d - 1], peer_of(d))
            for d in (2, 1, 3)
        ]

    st = (st_s, st_r)
    fwd_x = row_sends(sx, st, 0, x_peer, x) + row_sends(mx, st, 3, x_peer, x)
    loads[5].wait()
    queries_f = project(3)
    for h in range(NH):
        cols = slice(h * HD, (h + 1) * HD)
        unit_q = unit(h, queries_f)
        sq[:, cols] = unit_q.astype(BF16)
        startq[:, cols] = (unit_q * jnp.exp(ccol[h])).astype(BF16)

    def piece(idx, yy, xx, lo, size, to, slots=slice(0, 2)):
        ref = lat.at[yy % 4, xx % 4, slots, pl.ds(pl.multiple_of(hb + lo, 64), size), :]
        return remote(ref, ref, gs.at[idx], gr.at[idx], to)

    level_2 = [
        piece(4, y, x - 1, 0, 128, xp),
        piece(5, y, x + 1, 128, 128, xm),
        piece(6, y - 1, x, 0, 128, yp),
        piece(7, y + 1, x, 128, 128, ym),
        piece(8, y, x - 1, 0, 128, yp),
        piece(9, y, x - 1, 0, 128, ym),
        piece(10, y, x + 1, 0, 128, yp),
        piece(11, y, x + 1, 0, 128, ym),
        piece(12, y - 1, x, 128, 128, xp),
        piece(13, y - 1, x, 128, 128, xm),
        piece(14, y + 1, x, 128, 128, xp),
        piece(15, y + 1, x, 128, 128, xm),
    ]
    level_3 = [
        piece(16, y, x + 2, 0, 128, yp),
        piece(17, y, x + 2, 0, 128, ym),
        piece(18, y + 2, x, 128, 128, xp),
        piece(19, y + 2, x, 128, 128, xm),
        piece(20, y - 1, x - 1, 0, 64, yp),
        piece(21, y + 1, x - 1, 64, 64, ym),
        piece(22, y - 1, x + 1, 0, 64, yp),
        piece(23, y + 1, x + 1, 64, 64, ym),
        piece(24, y - 1, x - 1, 128, 64, xp),
        piece(25, y - 1, x + 1, 192, 64, xm),
        piece(26, y + 1, x - 1, 128, 64, xp),
        piece(27, y + 1, x + 1, 192, 64, xm),
    ]
    level_4 = [
        piece(28, y - 1, x + 2, 0, 64, yp),
        piece(29, y + 1, x + 2, 64, 64, ym),
        piece(30, y + 2, x - 1, 128, 64, xp),
        piece(31, y + 2, x + 1, 192, 64, xm),
    ]
    rest = slice(2, 4)
    rest_y = [piece(40, y - 1, x, 0, 128, yp, rest), piece(41, y + 1, x, 128, 128, ym, rest)]
    rest_x = [piece(42, y, x - 1, 0, 128, xp, rest), piece(43, y, x + 1, 128, 128, xm, rest)]
    levels = (sum(level_1, []), level_2, level_3, level_4)

    def to_partner(i, yy, xx):
        ref = lat.at[yy, xx, :, pl.ds(own, HALF), :]
        return remote(ref, ref, ds_.at[i], dr.at[i], partner)

    def other_slices(b, yy, xx):
        return (
            remote(slot(yy, xx, 0), slot(yy, xx, 3), zg_s.at[2 * b], zg_r.at[2 * b], z_peer(1)),
            remote(slot(yy, xx, 1), slot(yy, xx, 2), zg_s.at[2 * b + 1], zg_r.at[2 * b + 1], z_peer(3)),
        )

    def arrive(n):
        for copy in levels[n]:
            copy.wait_recv()
        if n < 3:
            for copy in levels[n + 1]:
                copy.start()
        for b in range(*LEVEL_OVER_Z[n]):
            for copy in other_slices(b, *away(b)):
                copy.start()

    def away(i):
        return (y + AWAY[i][0]) % 4, (x + AWAY[i][1]) % 4

    to_z[0].wait_recv()
    to_z[1].wait_recv()
    own_to_partner = to_partner(15, y, x)
    own_to_partner.start()
    arrive(0)

    for h in range(NH):
        cols = slice(h * HD, (h + 1) * HD)
        raw = nt(sq[:, cols], sk[:, cols])
        gaps = ccol[h, :, 0:1] - crow[h : h + 1, :]
        mix[h] = (raw * jnp.exp(jnp.where(col_at <= row_at, gaps, NEG_FILL))).astype(BF16)
    for h in range(NH):
        cols = slice(h * HD, (h + 1) * HD)
        sout[:, cols] = nn(mix[h], sv[:, cols])

    def stage(buf, decays, position, order, h):
        rows = slice(h * HD, (h + 1) * HD)
        running = jnp.zeros((HD, HD), F32)
        total = jnp.zeros((1, HD), F32)
        inside, inside_log = running, total
        for k in order:
            here = position == k
            inside = jnp.where(here, running, inside)
            inside_log = jnp.where(here, total, inside_log)
            log_decay = decays[k, h : h + 1, :]
            running = running * jnp.exp(log_decay) + buf[k, rows, :].astype(F32)
            total = total + log_decay
        return inside, inside_log, running, total

    rise, fall = (0, 1, 2, 3), (3, 2, 1, 0)
    fwd_y = row_sends(sy, st, 6, y_peer, y) + row_sends(my, st, 9, y_peer, y)

    def forward_row():
        for copy in fwd_x:
            copy.wait_recv()
        ends = []
        for h in range(NH):
            rows = slice(h * HD, (h + 1) * HD)
            inside, inside_log, running, total = stage(sx, mx, x, rise, h)
            held[rows, :] = inside
            heldlog[h : h + 1, :] = inside_log
            sy[y, rows, :] = running.astype(BF16)
            ends.append(total)
        my[y] = jnp.concatenate(ends + [blank], axis=0)
        for copy in fwd_y:
            copy.start()

    def tok_turn(i, carry):
        cut = pl.ds(pl.multiple_of(i * 256, 256), 256)
        tokt[cut, :] = jnp.transpose(tok[:, cut])
        return carry

    lax.fori_loop(0, D // 256, tok_turn, 0)

    for copy in loads[7:]:
        copy.wait()
    wvt[...] = jnp.transpose(wv[...])
    for h in range(NH):
        vt[h, HD:, :] = jnp.ones((ONES, 2 * T), BF16)

    def attend(blocks, masked=False):
        keys = T * len(blocks)
        arrays = []
        for n, (yy, xx) in enumerate(blocks):
            block = jnp.concatenate([lat[yy, xx, k] for k in range(4)], axis=1)
            kbuf[n * T : (n + 1) * T, :] = nn(block, wk[...]).astype(BF16)
            arrays.append(block)
        scores = [
            nt(kbuf[0:keys, h * HD : (h + 1) * HD], qbuf[:, h * HD : (h + 1) * HD]) for h in range(NH)
        ]
        for n, block in enumerate(arrays):
            values = nt(wvt[...], block).astype(BF16)
            for h in range(NH):
                vt[h, 0:HD, n * T : (n + 1) * T] = values[h * HD : (h + 1) * HD, :]
        for h in range(NH):
            score = scores[h]
            if masked:
                score = jnp.where(row_at <= col_at, score, NEG_FILL)
            best = jnp.max(score, axis=0, keepdims=True)
            if not masked:
                old = mrun[h : h + 1, :]
                best = jnp.maximum(old, best)
            weights = jnp.exp2((score - best) * EXP2_SCALE).astype(BF16)
            part = nn(vt[h, :, 0:keys], weights)
            if not masked:
                part += acc[h] * jnp.exp2((old - best) * EXP2_SCALE)
            acc[h] = part
            mrun[h : h + 1, :] = best

    own_to_partner.wait_recv()
    attend([(y, x)], masked=True)

    def place(b):
        yy = (y + pick(b, [a[0] for a in AWAY]) + 4) % 4
        xx = (x + pick(b, [a[1] for a in AWAY]) + 4) % 4
        return yy, xx

    def pass_on(b):
        yy, xx = place(b)
        for copy in other_slices(b, yy, xx):
            copy.wait_recv()
        to_partner(b, yy, xx).start()

    pass_on(0)
    pass_on(1)
    for copy in rest_y:
        copy.start()

    def block_step(i, carry):
        for n in (1, 2, 3):

            @pl.when(i == LEVEL_STEP[n])
            def _():
                arrive(n)
                if n == 1:
                    for copy in fwd_x:
                        copy.start()
                if n == 3:
                    forward_row()

        @pl.when(jnp.logical_and(i < 7, i != 3))
        def _():
            pass_on(2 * i + 2)

        @pl.when(jnp.logical_and(i < 6, i != 3))
        def _():
            pass_on(2 * i + 3)

        @pl.when(i == 0)
        def _():
            for copy in rest_x:
                copy.start()

        @pl.when(i == 3)
        def _():
            for b, copies in ((8, rest_y), (9, rest_x)):
                for copy in copies:
                    copy.wait_recv()
                to_partner(b, *away(b)).start()

        y1, x1 = place(2 * i)
        to_partner(2 * i, y1, x1).wait_recv()
        y2, x2 = place(2 * i + 1)

        @pl.when(i < 7)
        def _():
            to_partner(2 * i + 1, y2, x2).wait_recv()

        need_1 = y1 * 4 + x1 < s
        need_2 = jnp.logical_and(y2 * 4 + x2 < s, i < 7)

        @pl.when(jnp.logical_and(need_1, need_2))
        def _():
            attend([(y1, x1), (y2, x2)])

        @pl.when(need_1 != need_2)
        def _():
            attend([(jnp.where(need_1, y1, y2), jnp.where(need_1, x1, x2))])

        return carry

    lax.fori_loop(0, 8, block_step, 0)

    for copy in fwd_y:
        copy.wait_recv()
    for h in range(NH):
        cols = slice(h * HD, (h + 1) * HD)
        inside_y = stage(sy, my, y, rise, h)[0]
        prefix = (held[cols, :] + jnp.exp(heldlog[h : h + 1, :]) * inside_y).astype(BF16)
        sout[:, cols] = sout[:, cols] + nn(startq[:, cols], prefix)

    def head_sends(buf, first, peer_of, slot, h):
        ref = buf.at[slot, h * HD : (h + 1) * HD, :]
        at = [first + 3 * h + d - 1 for d in (2, 1, 3)]
        return [remote(ref, ref, st_s.at[k], st_r.at[k], peer_of(d)) for k, d in zip(at, (2, 1, 3))]

    back_x = [head_sends(bx, 12, x_peer, x, h) for h in range(NH)]
    back_y = [head_sends(by, 18, y_peer, y, h) for h in range(NH)]
    squares = jnp.zeros((8, HD), F32)
    inv = 1.0 / math.sqrt(ALL_TOKENS)
    for h in range(NH):
        cols = slice(h * HD, (h + 1) * HD)
        teacher = jnp.transpose(acc[h, 0:HD, :] / acc[h, HD : HD + 1, :]).astype(BF16)
        tout_ref[:, cols] = teacher
        mismatch = sout[:, cols] - teacher.astype(F32)
        squares += jnp.sum((mismatch * mismatch).reshape(T // 8, 8, HD), axis=0)
        vg[:, cols] = (mismatch * inv).astype(BF16)
        bx[x, cols, :] = tn(startq[:, cols], vg[:, cols]).astype(BF16)
        for copy in back_x[h]:
            copy.start()
    lx[x] = squares
    ls = (ls_s, ls_r)
    loss_x = row_sends(lx, ls, 0, x_peer, x)
    for copy in loss_x:
        copy.start()
    for h in range(NH):
        cols = slice(h * HD, (h + 1) * HD)
        sout[:, cols] = tn(mix[h], vg[:, cols])

    row_inside = []
    for h in range(NH):
        for copy in back_x[h]:
            copy.wait_recv()
        inside, inside_log, running, _ = stage(bx, mx, x, fall, h)
        row_inside.append((inside, inside_log))
        by[y, h * HD : (h + 1) * HD, :] = running.astype(BF16)
        for copy in back_y[h]:
            copy.start()
    for copy in loss_x:
        copy.wait_recv()
    ly[y] = lx[0] + lx[1] + lx[2] + lx[3]
    loss_y = row_sends(ly, ls, 3, y_peer, y)
    for copy in loss_y:
        copy.start()

    def value_gradient(h):
        cols = slice(h * HD, (h + 1) * HD)
        for copy in back_y[h]:
            copy.wait_recv()
        inside_y = stage(by, my, y, fall, h)[0]
        inside, inside_log = row_inside[h]
        suffix = (inside + jnp.exp(inside_log) * inside_y).astype(BF16)
        vg[:, cols] = (sout[:, cols] + nn(endk[:, cols], suffix)).astype(BF16)

    def weight_gradient(h):
        values = vg[:, h * HD : (h + 1) * HD]
        for i in range(4):
            part = nn(tokt[i * 512 : (i + 1) * 512, :], values).astype(BF16)
            for k in range(4):
                pw[h, i, k] = part[k * 128 : (k + 1) * 128, :]

    rs_x1 = [
        remote(pw.at[0, :, (x + d) % 4], r1in.at[0, d - 1], rs_s.at[d - 1], rs_r.at[d - 1], x_peer(d))
        for d in (2, 1, 3)
    ]
    rs_y1 = [
        remote(pw.at[1, (y + d) % 4], r1in.at[1, d - 1], rs_s.at[d + 2], rs_r.at[d + 2], y_peer(d))
        for d in (2, 1, 3)
    ]
    value_gradient(0)
    weight_gradient(0)
    for copy in rs_x1:
        copy.start()
    value_gradient(1)
    weight_gradient(1)
    for copy in rs_y1:
        copy.start()
    for copy in loss_y:
        copy.wait_recv()
    lz[z] = ly[0] + ly[1] + ly[2] + ly[3]
    loss_z = row_sends(lz, ls, 6, z_peer, z)
    for copy in loss_z:
        copy.start()

    for copy in rs_x1:
        copy.wait_recv()
    mine = [pw[0, k, x].astype(F32) for k in range(4)]
    for k in range(4):
        r1own[0, k] = (mine[k] + sum(r1in[0, d, k].astype(F32) for d in range(3))).astype(BF16)
    rs_y2 = [
        remote(r1own.at[0, (y + d) % 4], r2in.at[0, d - 1], rs_s.at[d + 5], rs_r.at[d + 5], y_peer(d))
        for d in (2, 1, 3)
    ]
    for copy in rs_y2:
        copy.start()
    for copy in rs_y1:
        copy.wait_recv()
    mine = [pw[1, y, k].astype(F32) for k in range(4)]
    for k in range(4):
        r1own[1, k] = (mine[k] + sum(r1in[1, d, k].astype(F32) for d in range(3))).astype(BF16)
    rs_x2 = [
        remote(r1own.at[1, (x + d) % 4], r2in.at[1, d - 1], rs_s.at[d + 8], rs_r.at[d + 8], x_peer(d))
        for d in (2, 1, 3)
    ]
    for copy in rs_x2:
        copy.start()

    for copy in loss_z:
        copy.wait_recv()
    lc[c] = lz[0] + lz[1] + lz[2] + lz[3]
    loss_c = remote(lc.at[c], lc.at[c], ls_s.at[9], ls_r.at[9], partner)
    loss_c.start()
    loss_c.wait_recv()
    loss_ref[0, 0] = jnp.sum(lc[0] + lc[1]) / (2.0 * ALL_TOKENS * ALL_HEADS * HD)

    for copy in rs_y2:
        copy.wait_recv()
    wg_ref[:, 0:HD] = r1own[0, y].astype(F32) + sum(r2in[0, d].astype(F32) for d in range(3))
    for copy in rs_x2:
        copy.wait_recv()
    wg_ref[:, HD:W] = r1own[1, x].astype(F32) + sum(r2in[1, d].astype(F32) for d in range(3))

    sent = [to_pair] + to_z + fwd_x + fwd_y + sum(back_x + back_y, [])
    sent += loss_x + loss_y + loss_z + [loss_c] + rs_x1 + rs_y1 + rs_y2 + rs_x2
    for level in levels:
        sent += level
    for b in range(15):
        sent += [to_partner(b, *away(b))]
    for first, last in LEVEL_OVER_Z:
        for b in range(first, last):
            sent += other_slices(b, *away(b))
    sent += rest_x + rest_y
    sent.append(own_to_partner)
    for copy in sent:
        copy.wait_send()


def finish(teacher_ref, wgrad_ref, teacher_out, wgrad_out, sem):
    copies = [
        pltpu.make_async_copy(teacher_ref, teacher_out, sem.at[0]),
        pltpu.make_async_copy(wgrad_ref, wgrad_out, sem.at[1]),
    ]
    for copy in copies:
        copy.start()
    for copy in copies:
        copy.wait()


def per_device(tokens, w_latent, w_query, w_key_up, w_value_up, w_stu_query, w_stu_key, w_stu_value, forget):
    dma = pltpu.SemaphoreType.DMA
    scratch = [
        pltpu.VMEM((T, D), BF16),
        pltpu.VMEM((D, T), BF16),
        pltpu.VMEM((HD, D), BF16),
        pltpu.VMEM((4, D, W), BF16),
        pltpu.VMEM((LAT, W), BF16),
        pltpu.VMEM((LAT, W), BF16),
        pltpu.VMEM((W, LAT), BF16),
        pltpu.VMEM((NH, T), F32),
        pltpu.VMEM((4, 4, 4, T, HD), BF16),
        pltpu.VMEM((T, HD), BF16),
        pltpu.VMEM((HALF, HD), BF16),
        pltpu.VMEM((HALF, HD), BF16),
        pltpu.VMEM((2 * T, W), BF16),
        pltpu.VMEM((NH, HD + ONES, 2 * T), BF16),
        pltpu.VMEM((T, W), BF16),
        pltpu.VMEM((NH, HD + ONES, T), F32),
        pltpu.VMEM((8, T), F32),
        pltpu.VMEM((T, W), BF16),
        pltpu.VMEM((T, W), BF16),
        pltpu.VMEM((T, W), BF16),
        pltpu.VMEM((NH, T, HD), F32),
        pltpu.VMEM((8, T), F32),
        pltpu.VMEM((NH, T, T), BF16),
        pltpu.VMEM((T, W), F32),
        pltpu.VMEM((T, W), BF16),
        pltpu.VMEM((T, W), BF16),
        pltpu.VMEM((T, W), BF16),
        pltpu.VMEM((W, HD), F32),
        pltpu.VMEM((8, HD), F32),
        pltpu.VMEM((4, W, HD), BF16),
        pltpu.VMEM((4, W, HD), BF16),
        pltpu.VMEM((4, 8, HD), F32),
        pltpu.VMEM((4, 8, HD), F32),
        pltpu.VMEM((4, W, HD), BF16),
        pltpu.VMEM((4, W, HD), BF16),
        pltpu.VMEM((4, 8, HD), F32),
        pltpu.VMEM((4, 8, HD), F32),
        pltpu.VMEM((4, 8, HD), F32),
        pltpu.VMEM((2, 8, HD), F32),
        pltpu.VMEM((NH, 4, 4, 128, HD), BF16),
        pltpu.VMEM((NH, 3, 4, 128, HD), BF16),
        pltpu.VMEM((NH, 4, 128, HD), BF16),
        pltpu.VMEM((NH, 3, 128, HD), BF16),
        dma((15,)),
        dma,
        dma,
        dma((3,)),
        dma((3,)),
        dma((44,)),
        dma((44,)),
        dma((30,)),
        dma((30,)),
        dma((16,)),
        dma((16,)),
        dma((24,)),
        dma((24,)),
        dma((12,)),
        dma((12,)),
        dma((10,)),
        dma((10,)),
    ]
    anywhere = pl.BlockSpec(memory_space=pl.ANY)
    teacher, loss, wgrad = pl.pallas_call(
        kernel,
        out_shape=(
            pltpu.VMEM((T, W), BF16),
            jax.ShapeDtypeStruct((1, 1), F32),
            pltpu.VMEM((128, W), F32),
        ),
        in_specs=[anywhere] * 9,
        out_specs=(
            pl.BlockSpec(memory_space=pltpu.VMEM),
            pl.BlockSpec(memory_space=pltpu.SMEM),
            pl.BlockSpec(memory_space=pltpu.VMEM),
        ),
        scratch_shapes=scratch,
        compiler_params=pltpu.CompilerParams(
            collective_id=0, has_side_effects=True, vmem_limit_bytes=60 * 1024 * 1024
        ),
    )(
        tokens, w_latent.T, w_query, w_key_up, w_value_up, w_stu_query, w_stu_key, w_stu_value, forget.T
    )
    teacher, wgrad = pl.pallas_call(
        finish,
        out_shape=(jax.ShapeDtypeStruct((T, W), BF16), jax.ShapeDtypeStruct((128, W), F32)),
        in_specs=[pl.BlockSpec(memory_space=pltpu.VMEM)] * 2,
        out_specs=(anywhere, anywhere),
        scratch_shapes=[dma((2,))],
        compiler_params=pltpu.CompilerParams(vmem_limit_bytes=4 * 1024 * 1024),
    )(teacher, wgrad)
    return teacher, loss[0, 0], wgrad


def solution(mesh):
    return jax.shard_map(
        per_device,
        mesh=mesh,
        in_specs=(
            P("seq", None),
            P(None, "tensor"),
            P(None, "tensor"),
            P(None, "tensor"),
            P(None, "tensor"),
            P(None, "tensor"),
            P(None, "tensor"),
            P(None, "tensor"),
            P("seq", "tensor"),
        ),
        out_specs=(P("seq", "tensor"), P(), P("seq", "tensor")),
        check_vma=False,
    )
```

```python
import math

import jax
import jax.numpy as jnp
from jax import lax
from jax.experimental import pallas as pl
from jax.experimental.pallas import tpu as pltpu
from jax.sharding import PartitionSpec as P

F32 = jnp.float32
BF16 = jnp.bfloat16
MESH = pl.DeviceIdType.MESH
NEG_FILL = -1e30
EPSILON = 1e-06

T = 512
D = 2048
HD = 128
NH = 2
W = NH * HD
LAT = 512
HALF = T // 2
ONES = 16
ALL_TOKENS = 8192
ALL_HEADS = 16
EXP2_SCALE = math.log2(math.e) / math.sqrt(HD)

AWAY = (
    (-1, 0), (1, 0), (0, -1), (0, 1),
    (-1, -1), (1, -1), (-1, 1), (1, 1),
    (2, 0), (0, 2),
    (-1, 2), (1, 2), (2, -1), (2, 1),
    (2, 2),
)
LEVEL_OVER_Z = ((0, 4), (4, 8), (10, 14), (14, 15))
LEVEL_STEP = (None, None, 2, 4)


def nt(a, b):
    return lax.dot_general(a, b, (((1,), (1,)), ((), ())), preferred_element_type=F32)


def nn(a, b):
    return jnp.dot(a, b, preferred_element_type=F32)


def tn(a, b):
    return lax.dot_general(a, b, (((0,), (0,)), ((), ())), preferred_element_type=F32)


def pick(index, values):
    out = jnp.int32(values[0])
    for k in range(1, len(values)):
        out = jnp.where(index == k, jnp.int32(values[k]), out)
    return out


def three_parts(a):
    hi = a.astype(BF16)
    rest = a - hi.astype(F32)
    mid = rest.astype(BF16)
    low = (rest - mid.astype(F32)).astype(BF16)
    return hi, mid, low


def kernel(
    tok_h, wl_h, wq_h, wku_h, wvu_h, wsq_h, wsk_h, wsv_h, fg_h,
    tout_ref, loss_ref, wg_ref,
    tok, tokt, wl, wall, wk, wv, wvt, fgv,
    lat, myp, pairin, pairbuf, kbuf, vt, qbuf, acc, mrun,
    sq, sk, sv, ccol, crow, mix, sout, startq, endk, vg,
    held, heldlog, sx, sy, mx, my, bx, by, lx, ly, lz, lc,
    pw, r1in, r1own, r2in, gw, gwin, hrow, lown, lin,
    load_sem, pair_s, pair_r, z_s, z_r, gs, gr, zg_s, zg_r, ds_, dr,
    st_s, st_r, rs_s, rs_r, ls_s, ls_r, gw_s, gw_r,
):
    s = lax.axis_index("seq")
    t = lax.axis_index("tensor")
    y, x = s // 4, s % 4
    z, c = t // 2, t % 2
    hb = c * HALF

    def plane(yy, xx):
        return (yy * 4 + xx, t)

    def x_peer(d):
        return plane(y, (x + d) % 4)

    def y_peer(d):
        return plane((y + d) % 4, x)

    def z_peer(d):
        return (s, ((z + d) % 4) * 2 + c)

    partner = (s, z * 2 + (1 - c))

    def remote(src, dst, send, recv, to):
        return pltpu.make_async_remote_copy(
            src_ref=src, dst_ref=dst, send_sem=send, recv_sem=recv, device_id=to, device_id_type=MESH
        )

    wl[...] = jnp.zeros_like(wl)
    loads = [
        pltpu.make_async_copy(wl_h, wl.at[pl.ds(pl.multiple_of(c * 64, 64), 64), :], load_sem.at[0]),
        pltpu.make_async_copy(tok_h, tok, load_sem.at[1]),
        pltpu.make_async_copy(wq_h, wall.at[0], load_sem.at[2]),
        pltpu.make_async_copy(wsk_h, wall.at[1], load_sem.at[3]),
        pltpu.make_async_copy(wsv_h, wall.at[2], load_sem.at[4]),
        pltpu.make_async_copy(wsq_h, wall.at[3], load_sem.at[5]),
        pltpu.make_async_copy(fg_h, fgv, load_sem.at[6]),
    ]
    for j in range(4):
        rows = pl.ds(pl.multiple_of((z + j) % 4 * HD, HD), HD)
        loads.append(pltpu.make_async_copy(wku_h.at[rows, :], wk.at[j * HD : (j + 1) * HD, :], load_sem.at[7 + j]))
        loads.append(pltpu.make_async_copy(wvu_h.at[rows, :], wv.at[j * HD : (j + 1) * HD, :], load_sem.at[11 + j]))
    loads[0].start()
    loads[1].start()
    barrier = pltpu.get_barrier_semaphore()
    peers = [x_peer(d) for d in (1, 2, 3)] + [y_peer(d) for d in (1, 2, 3)]
    peers += [z_peer(d) for d in (1, 2, 3)] + [partner]
    for peer in peers:
        pl.semaphore_signal(barrier, inc=1, device_id=peer, device_id_type=MESH)

    loads[0].wait()
    loads[1].wait()
    for copy in loads[2:]:
        copy.start()
    myp[...] = nt(tok[...], wl[...]).astype(BF16)
    pl.semaphore_wait(barrier, 10)
    other = pl.multiple_of((1 - c) * HALF, HALF)
    own = pl.multiple_of(hb, HALF)
    to_pair = remote(myp.at[pl.ds(other, HALF), :], pairin, pair_s, pair_r, partner)
    to_pair.start()

    def project(i):
        return nn(tok[...], wall[i])

    loads[2].wait()
    qbuf[...] = project(0).astype(BF16)
    to_pair.wait_recv()
    pairbuf[...] = myp[pl.ds(own, HALF), :] + pairin[...]
    my_slice = lat.at[y, x, z, pl.ds(own, HALF), :]
    lat[y, x, 0, pl.ds(own, HALF), :] = pairbuf[...]

    def slot(yy, xx, j):
        return lat.at[yy, xx, j, pl.ds(own, HALF), :]

    to_z = [
        remote(pairbuf, slot(y, x, 4 - d), z_s.at[d - 1], z_r.at[d - 1], z_peer(d)) for d in (1, 2, 3)
    ]
    for d in (3, 1, 2):
        to_z[d - 1].start()
    xp, xm, yp, ym = x_peer(1), x_peer(3), y_peer(1), y_peer(3)

    def near(j):
        return [
            remote(slot(y, x, j), slot(y, x, j), gs.at[32 + 2 * k + j], gr.at[32 + 2 * k + j], to)
            for k, to in enumerate((yp, ym, xp, xm))
        ]

    level_1 = [near(0), near(1)]
    for copy in level_1[0]:
        copy.start()

    def unit(h, m):
        part = m[:, h * HD : (h + 1) * HD]
        return part * lax.rsqrt(jnp.sum(part * part, axis=-1, keepdims=True) + EPSILON)

    loads[6].wait()
    row_at = lax.broadcasted_iota(jnp.int32, (T, T), 0)
    col_at = lax.broadcasted_iota(jnp.int32, (T, T), 1)
    lower = (col_at <= row_at).astype(BF16)
    f_parts = three_parts(fgv[...])
    crow[0:NH, :] = sum(nt(part, lower) for part in f_parts)
    for h in range(NH):
        spread = [jnp.broadcast_to(part[h : h + 1, :], (HD, T)) for part in f_parts]
        ccol[h] = sum(nt(lower, part) for part in spread)

    loads[3].wait()
    keys_f = project(1)
    loads[4].wait()
    sv[...] = project(2).astype(BF16)
    to_z[2].wait_recv()
    for copy in level_1[1]:
        copy.start()
    ends = []
    for h in range(NH):
        cols = slice(h * HD, (h + 1) * HD)
        unit_k = unit(h, keys_f)
        sk[:, cols] = unit_k.astype(BF16)
        end_row = ccol[h, T - 1 : T, :]
        endk[:, cols] = (unit_k * jnp.exp(end_row - ccol[h])).astype(BF16)
        ends.append(end_row)
    blank = jnp.zeros((8 - NH, HD), F32)
    mx[x] = jnp.concatenate(ends + [blank], axis=0)
    for h in range(NH):
        cols = slice(h * HD, (h + 1) * HD)
        sx[x, cols, :] = tn(endk[:, cols], sv[:, cols]).astype(BF16)

    def row_sends(buf, sems, first, peer_of, slot):
        return [
            remote(buf.at[slot], buf.at[slot], sems[0].at[first + d - 1], sems[1].at[first + d - 1], peer_of(d))
            for d in (2, 1, 3)
        ]

    st = (st_s, st_r)
    fwd_x = row_sends(sx, st, 0, x_peer, x)
    ends_x = row_sends(mx, st, 3, x_peer, x)
    for copy in ends_x:
        copy.start()
    loads[5].wait()
    queries_f = project(3)
    for h in range(NH):
        cols = slice(h * HD, (h + 1) * HD)
        unit_q = unit(h, queries_f)
        sq[:, cols] = unit_q.astype(BF16)
        startq[:, cols] = (unit_q * jnp.exp(ccol[h])).astype(BF16)

    def piece(idx, yy, xx, lo, size, to, slots=slice(0, 2)):
        ref = lat.at[yy % 4, xx % 4, slots, pl.ds(pl.multiple_of(hb + lo, 64), size), :]
        return remote(ref, ref, gs.at[idx], gr.at[idx], to)

    level_2 = [
        piece(4, y, x - 1, 0, 128, xp),
        piece(5, y, x + 1, 128, 128, xm),
        piece(6, y - 1, x, 0, 128, yp),
        piece(7, y + 1, x, 128, 128, ym),
        piece(8, y, x - 1, 0, 128, yp),
        piece(9, y, x - 1, 0, 128, ym),
        piece(10, y, x + 1, 0, 128, yp),
        piece(11, y, x + 1, 0, 128, ym),
        piece(12, y - 1, x, 128, 128, xp),
        piece(13, y - 1, x, 128, 128, xm),
        piece(14, y + 1, x, 128, 128, xp),
        piece(15, y + 1, x, 128, 128, xm),
    ]
    level_3 = [
        piece(16, y, x + 2, 0, 128, yp),
        piece(17, y, x + 2, 0, 128, ym),
        piece(18, y + 2, x, 128, 128, xp),
        piece(19, y + 2, x, 128, 128, xm),
        piece(20, y - 1, x - 1, 0, 64, yp),
        piece(21, y + 1, x - 1, 64, 64, ym),
        piece(22, y - 1, x + 1, 0, 64, yp),
        piece(23, y + 1, x + 1, 64, 64, ym),
        piece(24, y - 1, x - 1, 128, 64, xp),
        piece(25, y - 1, x + 1, 192, 64, xm),
        piece(26, y + 1, x - 1, 128, 64, xp),
        piece(27, y + 1, x + 1, 192, 64, xm),
    ]
    level_4 = [
        piece(28, y - 1, x + 2, 0, 64, yp),
        piece(29, y + 1, x + 2, 64, 64, ym),
        piece(30, y + 2, x - 1, 128, 64, xp),
        piece(31, y + 2, x + 1, 192, 64, xm),
    ]
    rest = slice(2, 4)
    rest_y = [piece(40, y - 1, x, 0, 128, yp, rest), piece(41, y + 1, x, 128, 128, ym, rest)]
    rest_x = [piece(42, y, x - 1, 0, 128, xp, rest), piece(43, y, x + 1, 128, 128, xm, rest)]
    levels = (sum(level_1, []), level_2, level_3, level_4)

    def to_partner(i, yy, xx):
        ref = lat.at[yy, xx, :, pl.ds(own, HALF), :]
        return remote(ref, ref, ds_.at[i], dr.at[i], partner)

    def other_slices(b, yy, xx):
        return (
            remote(slot(yy, xx, 0), slot(yy, xx, 3), zg_s.at[2 * b], zg_r.at[2 * b], z_peer(1)),
            remote(slot(yy, xx, 1), slot(yy, xx, 2), zg_s.at[2 * b + 1], zg_r.at[2 * b + 1], z_peer(3)),
        )

    def arrive(n):
        for copy in levels[n]:
            copy.wait_recv()
        if n < 3:
            for copy in levels[n + 1]:
                copy.start()
        for b in range(*LEVEL_OVER_Z[n]):
            for copy in other_slices(b, *away(b)):
                copy.start()

    def away(i):
        return (y + AWAY[i][0]) % 4, (x + AWAY[i][1]) % 4

    to_z[0].wait_recv()
    to_z[1].wait_recv()
    own_to_partner = to_partner(15, y, x)
    own_to_partner.start()
    arrive(0)

    for h in range(NH):
        cols = slice(h * HD, (h + 1) * HD)
        raw = nt(sq[:, cols], sk[:, cols])
        gaps = ccol[h, :, 0:1] - crow[h : h + 1, :]
        mix[h] = (raw * jnp.exp(jnp.where(col_at <= row_at, gaps, NEG_FILL))).astype(BF16)
    for h in range(NH):
        cols = slice(h * HD, (h + 1) * HD)
        sout[:, cols] = nn(mix[h], sv[:, cols])

    def stage(buf, decays, position, order, h):
        rows = slice(h * HD, (h + 1) * HD)
        running = jnp.zeros((HD, HD), F32)
        total = jnp.zeros((1, HD), F32)
        inside, inside_log = running, total
        for k in order:
            here = position == k
            inside = jnp.where(here, running, inside)
            inside_log = jnp.where(here, total, inside_log)
            log_decay = decays[k, h : h + 1, :]
            running = running * jnp.exp(log_decay) + buf[k, rows, :].astype(F32)
            total = total + log_decay
        return inside, inside_log, running, total

    rise, fall = (0, 1, 2, 3), (3, 2, 1, 0)
    fwd_y = row_sends(sy, st, 6, y_peer, y) + row_sends(my, st, 9, y_peer, y)

    def forward_row():
        for copy in fwd_x:
            copy.wait_recv()
        ends = []
        for h in range(NH):
            rows = slice(h * HD, (h + 1) * HD)
            inside, inside_log, running, total = stage(sx, mx, x, rise, h)
            held[rows, :] = inside
            heldlog[h : h + 1, :] = inside_log
            sy[y, rows, :] = running.astype(BF16)
            ends.append(total)
        my[y] = jnp.concatenate(ends + [blank], axis=0)
        for copy in fwd_y:
            copy.start()

    def tok_turn(i, carry):
        cut = pl.ds(pl.multiple_of(i * 256, 256), 256)
        tokt[cut, :] = jnp.transpose(tok[:, cut])
        return carry

    lax.fori_loop(0, D // 256, tok_turn, 0)

    for copy in loads[7:]:
        copy.wait()
    wvt[...] = jnp.transpose(wv[...])
    for h in range(NH):
        vt[h, HD:, :] = jnp.ones((ONES, 2 * T), BF16)

    def attend(blocks, masked=False):
        keys = T * len(blocks)
        arrays = []
        for n, (yy, xx) in enumerate(blocks):
            block = jnp.concatenate([lat[yy, xx, k] for k in range(4)], axis=1)
            kbuf[n * T : (n + 1) * T, :] = nn(block, wk[...]).astype(BF16)
            arrays.append(block)
        scores = [
            nt(kbuf[0:keys, h * HD : (h + 1) * HD], qbuf[:, h * HD : (h + 1) * HD]) for h in range(NH)
        ]
        for n, block in enumerate(arrays):
            values = nt(wvt[...], block).astype(BF16)
            for h in range(NH):
                vt[h, 0:HD, n * T : (n + 1) * T] = values[h * HD : (h + 1) * HD, :]
        for h in range(NH):
            score = scores[h]
            if masked:
                score = jnp.where(row_at <= col_at, score, NEG_FILL)
            best = jnp.max(score, axis=0, keepdims=True)
            if not masked:
                old = mrun[h : h + 1, :]
                best = jnp.maximum(old, best)
            weights = jnp.exp2((score - best) * EXP2_SCALE).astype(BF16)
            part = nn(vt[h, :, 0:keys], weights)
            if not masked:
                part += acc[h] * jnp.exp2((old - best) * EXP2_SCALE)
            acc[h] = part
            mrun[h : h + 1, :] = best

    own_to_partner.wait_recv()
    attend([(y, x)], masked=True)

    def place(b):
        yy = (y + pick(b, [a[0] for a in AWAY]) + 4) % 4
        xx = (x + pick(b, [a[1] for a in AWAY]) + 4) % 4
        return yy, xx

    def pass_on(b):
        yy, xx = place(b)
        for copy in other_slices(b, yy, xx):
            copy.wait_recv()
        to_partner(b, yy, xx).start()

    for copy in ends_x:
        copy.wait_recv()
    for h in range(NH):
        cols = slice(h * HD, (h + 1) * HD)
        to_end = sum(jnp.where(x < k, mx[k, h : h + 1, :], 0.0) for k in (1, 2, 3))
        faded = (endk[:, cols].astype(F32) * jnp.exp(to_end)).astype(BF16)
        for i in range(4):
            part = nn(tokt[i * 512 : (i + 1) * 512, :], faded).astype(BF16)
            for k in range(4):
                gw[h, i, k] = part[k * 128 : (k + 1) * 128, :]
    row_gw = [
        [
            remote(gw.at[h, :, (x + d) % 4], gwin.at[h, d - 1], gw_s.at[3 * h + d - 1], gw_r.at[3 * h + d - 1], x_peer(d))
            for d in (2, 1, 3)
        ]
        for h in range(NH)
    ]
    arrive(1)
    for copy in fwd_x:
        copy.start()
    pass_on(0)
    pass_on(1)
    for copy in rest_y:
        copy.start()

    def block_step(i, carry):
        for n in (2, 3):

            @pl.when(i == LEVEL_STEP[n])
            def _():
                arrive(n)
                for copy in row_gw[n - 2]:
                    copy.start()
                if n == 3:
                    forward_row()

        @pl.when(jnp.logical_and(i < 7, i != 3))
        def _():
            pass_on(2 * i + 2)

        @pl.when(jnp.logical_and(i < 6, i != 3))
        def _():
            pass_on(2 * i + 3)

        @pl.when(i == 0)
        def _():
            for copy in rest_x:
                copy.start()

        @pl.when(i == 3)
        def _():
            for b, copies in ((8, rest_y), (9, rest_x)):
                for copy in copies:
                    copy.wait_recv()
                to_partner(b, *away(b)).start()

        y1, x1 = place(2 * i)
        to_partner(2 * i, y1, x1).wait_recv()
        y2, x2 = place(2 * i + 1)

        @pl.when(i < 7)
        def _():
            to_partner(2 * i + 1, y2, x2).wait_recv()

        need_1 = y1 * 4 + x1 < s
        need_2 = jnp.logical_and(y2 * 4 + x2 < s, i < 7)

        @pl.when(jnp.logical_and(need_1, need_2))
        def _():
            attend([(y1, x1), (y2, x2)])

        @pl.when(need_1 != need_2)
        def _():
            attend([(jnp.where(need_1, y1, y2), jnp.where(need_1, x1, x2))])

        return carry

    lax.fori_loop(0, 8, block_step, 0)

    for copy in fwd_y:
        copy.wait_recv()
    for h in range(NH):
        cols = slice(h * HD, (h + 1) * HD)
        inside_y = stage(sy, my, y, rise, h)[0]
        prefix = (held[cols, :] + jnp.exp(heldlog[h : h + 1, :]) * inside_y).astype(BF16)
        sout[:, cols] = sout[:, cols] + nn(startq[:, cols], prefix)

    def head_sends(buf, first, peer_of, slot, h):
        ref = buf.at[slot, h * HD : (h + 1) * HD, :]
        at = [first + 3 * h + d - 1 for d in (2, 1, 3)]
        return [remote(ref, ref, st_s.at[k], st_r.at[k], peer_of(d)) for k, d in zip(at, (2, 1, 3))]

    back_x = [head_sends(bx, 12, x_peer, x, h) for h in range(NH)]
    back_y = [head_sends(by, 18, y_peer, y, h) for h in range(NH)]
    squares = jnp.zeros((8, HD), F32)
    inv = 1.0 / math.sqrt(ALL_TOKENS)
    for h in range(NH):
        cols = slice(h * HD, (h + 1) * HD)
        teacher = jnp.transpose(acc[h, 0:HD, :] / acc[h, HD : HD + 1, :]).astype(BF16)
        tout_ref[:, cols] = teacher
        mismatch = sout[:, cols] - teacher.astype(F32)
        squares += jnp.sum((mismatch * mismatch).reshape(T // 8, 8, HD), axis=0)
        vg[:, cols] = (mismatch * inv).astype(BF16)
        bx[x, cols, :] = tn(startq[:, cols], vg[:, cols]).astype(BF16)
        for copy in back_x[h]:
            copy.start()
    lx[x] = squares
    ls = (ls_s, ls_r)
    loss_x = row_sends(lx, ls, 0, x_peer, x)
    for copy in loss_x:
        copy.start()
    for h in range(NH):
        cols = slice(h * HD, (h + 1) * HD)
        sout[:, cols] = tn(mix[h], vg[:, cols])

    for h in range(NH):
        for copy in row_gw[h]:
            copy.wait_recv()
        for k in range(4):
            total = gw[h, k, x].astype(F32) + sum(gwin[h, d, k].astype(F32) for d in range(3))
            hrow[h, k * 128 : (k + 1) * 128, :] = total.astype(BF16)
    row_inside = []
    for h in range(NH):
        for copy in back_x[h]:
            copy.wait_recv()
        inside, inside_log, running, _ = stage(bx, mx, x, fall, h)
        row_inside.append(inside.astype(BF16))
        by[y, h * HD : (h + 1) * HD, :] = running.astype(BF16)
        for copy in back_y[h]:
            copy.start()
    for copy in loss_x:
        copy.wait_recv()
    ly[y] = lx[0] + lx[1] + lx[2] + lx[3]
    loss_y = row_sends(ly, ls, 3, y_peer, y)
    for copy in loss_y:
        copy.start()

    def value_gradient(h):
        cols = slice(h * HD, (h + 1) * HD)
        vg[:, cols] = (sout[:, cols] + nn(endk[:, cols], row_inside[h])).astype(BF16)

    def from_later_rows(h):
        for copy in back_y[h]:
            copy.wait_recv()
        return nn(hrow[h], stage(by, my, y, fall, h)[0].astype(BF16))

    def weight_gradient(h):
        values = vg[:, h * HD : (h + 1) * HD]
        for i in range(4):
            part = nn(tokt[i * 512 : (i + 1) * 512, :], values).astype(BF16)
            for k in range(4):
                pw[h, i, k] = part[k * 128 : (k + 1) * 128, :]

    rs_x1 = [
        remote(pw.at[0, :, (x + d) % 4], r1in.at[0, d - 1], rs_s.at[d - 1], rs_r.at[d - 1], x_peer(d))
        for d in (2, 1, 3)
    ]
    rs_y1 = [
        remote(pw.at[1, (y + d) % 4], r1in.at[1, d - 1], rs_s.at[d + 2], rs_r.at[d + 2], y_peer(d))
        for d in (2, 1, 3)
    ]
    value_gradient(0)
    weight_gradient(0)
    for copy in rs_x1:
        copy.start()
    value_gradient(1)
    weight_gradient(1)
    for copy in rs_y1:
        copy.start()
    later = from_later_rows(0)
    later_1 = from_later_rows(1)
    for k in range(4):
        lown[k] = later_1[k * 128 : (k + 1) * 128, :].astype(BF16)
    rows_y = [
        remote(lown.at[(y + d) % 4], lin.at[d - 1], rs_s.at[d + 11], rs_r.at[d + 11], y_peer(d)) for d in (2, 1, 3)
    ]
    for copy in rows_y:
        copy.start()
    for copy in loss_y:
        copy.wait_recv()
    lz[z] = ly[0] + ly[1] + ly[2] + ly[3]
    loss_z = row_sends(lz, ls, 6, z_peer, z)
    for copy in loss_z:
        copy.start()

    for copy in rs_x1:
        copy.wait_recv()
    mine = [pw[0, k, x].astype(F32) for k in range(4)]
    for k in range(4):
        total = mine[k] + later[k * 128 : (k + 1) * 128, :]
        r1own[0, k] = (total + sum(r1in[0, d, k].astype(F32) for d in range(3))).astype(BF16)
    rs_y2 = [
        remote(r1own.at[0, (y + d) % 4], r2in.at[0, d - 1], rs_s.at[d + 5], rs_r.at[d + 5], y_peer(d))
        for d in (2, 1, 3)
    ]
    for copy in rs_y2:
        copy.start()
    for copy in rs_y1:
        copy.wait_recv()
    mine = [pw[1, y, k].astype(F32) for k in range(4)]
    for k in range(4):
        r1own[1, k] = (mine[k] + sum(r1in[1, d, k].astype(F32) for d in range(3))).astype(BF16)
    rs_x2 = [
        remote(r1own.at[1, (x + d) % 4], r2in.at[1, d - 1], rs_s.at[d + 8], rs_r.at[d + 8], x_peer(d))
        for d in (2, 1, 3)
    ]
    for copy in rs_x2:
        copy.start()

    for copy in loss_z:
        copy.wait_recv()
    lc[c] = lz[0] + lz[1] + lz[2] + lz[3]
    loss_c = remote(lc.at[c], lc.at[c], ls_s.at[9], ls_r.at[9], partner)
    loss_c.start()
    loss_c.wait_recv()
    loss_ref[0, 0] = jnp.sum(lc[0] + lc[1]) / (2.0 * ALL_TOKENS * ALL_HEADS * HD)

    for copy in rs_y2:
        copy.wait_recv()
    wg_ref[:, 0:HD] = r1own[0, y].astype(F32) + sum(r2in[0, d].astype(F32) for d in range(3))
    for copy in rows_y:
        copy.wait_recv()
    late = lown[y].astype(F32) + sum(lin[d].astype(F32) for d in range(3))
    for copy in rs_x2:
        copy.wait_recv()
    wg_ref[:, HD:W] = late + r1own[1, x].astype(F32) + sum(r2in[1, d].astype(F32) for d in range(3))

    sent = [to_pair] + to_z + fwd_x + fwd_y + sum(back_x + back_y, [])
    sent += loss_x + loss_y + loss_z + [loss_c] + rs_x1 + rs_y1 + rs_y2 + rs_x2
    sent += ends_x + sum(row_gw, []) + rows_y
    for level in levels:
        sent += level
    for b in range(15):
        sent += [to_partner(b, *away(b))]
    for first, last in LEVEL_OVER_Z:
        for b in range(first, last):
            sent += other_slices(b, *away(b))
    sent += rest_x + rest_y
    sent.append(own_to_partner)
    for copy in sent:
        copy.wait_send()


def finish(teacher_ref, wgrad_ref, teacher_out, wgrad_out, sem):
    copies = [
        pltpu.make_async_copy(teacher_ref, teacher_out, sem.at[0]),
        pltpu.make_async_copy(wgrad_ref, wgrad_out, sem.at[1]),
    ]
    for copy in copies:
        copy.start()
    for copy in copies:
        copy.wait()


def per_device(tokens, w_latent, w_query, w_key_up, w_value_up, w_stu_query, w_stu_key, w_stu_value, forget):
    dma = pltpu.SemaphoreType.DMA
    scratch = [
        pltpu.VMEM((T, D), BF16),
        pltpu.VMEM((D, T), BF16),
        pltpu.VMEM((HD, D), BF16),
        pltpu.VMEM((4, D, W), BF16),
        pltpu.VMEM((LAT, W), BF16),
        pltpu.VMEM((LAT, W), BF16),
        pltpu.VMEM((W, LAT), BF16),
        pltpu.VMEM((NH, T), F32),
        pltpu.VMEM((4, 4, 4, T, HD), BF16),
        pltpu.VMEM((T, HD), BF16),
        pltpu.VMEM((HALF, HD), BF16),
        pltpu.VMEM((HALF, HD), BF16),
        pltpu.VMEM((2 * T, W), BF16),
        pltpu.VMEM((NH, HD + ONES, 2 * T), BF16),
        pltpu.VMEM((T, W), BF16),
        pltpu.VMEM((NH, HD + ONES, T), F32),
        pltpu.VMEM((8, T), F32),
        pltpu.VMEM((T, W), BF16),
        pltpu.VMEM((T, W), BF16),
        pltpu.VMEM((T, W), BF16),
        pltpu.VMEM((NH, T, HD), F32),
        pltpu.VMEM((8, T), F32),
        pltpu.VMEM((NH, T, T), BF16),
        pltpu.VMEM((T, W), F32),
        pltpu.VMEM((T, W), BF16),
        pltpu.VMEM((T, W), BF16),
        pltpu.VMEM((T, W), BF16),
        pltpu.VMEM((W, HD), F32),
        pltpu.VMEM((8, HD), F32),
        pltpu.VMEM((4, W, HD), BF16),
        pltpu.VMEM((4, W, HD), BF16),
        pltpu.VMEM((4, 8, HD), F32),
        pltpu.VMEM((4, 8, HD), F32),
        pltpu.VMEM((4, W, HD), BF16),
        pltpu.VMEM((4, W, HD), BF16),
        pltpu.VMEM((4, 8, HD), F32),
        pltpu.VMEM((4, 8, HD), F32),
        pltpu.VMEM((4, 8, HD), F32),
        pltpu.VMEM((2, 8, HD), F32),
        pltpu.VMEM((NH, 4, 4, 128, HD), BF16),
        pltpu.VMEM((NH, 3, 4, 128, HD), BF16),
        pltpu.VMEM((NH, 4, 128, HD), BF16),
        pltpu.VMEM((NH, 3, 128, HD), BF16),
        pltpu.VMEM((NH, 4, 4, 128, HD), BF16),
        pltpu.VMEM((NH, 3, 4, 128, HD), BF16),
        pltpu.VMEM((NH, 512, HD), BF16),
        pltpu.VMEM((4, 128, HD), BF16),
        pltpu.VMEM((3, 128, HD), BF16),
        dma((15,)),
        dma,
        dma,
        dma((3,)),
        dma((3,)),
        dma((44,)),
        dma((44,)),
        dma((30,)),
        dma((30,)),
        dma((16,)),
        dma((16,)),
        dma((24,)),
        dma((24,)),
        dma((15,)),
        dma((15,)),
        dma((10,)),
        dma((10,)),
        dma((6,)),
        dma((6,)),
    ]
    anywhere = pl.BlockSpec(memory_space=pl.ANY)
    teacher, loss, wgrad = pl.pallas_call(
        kernel,
        out_shape=(
            pltpu.VMEM((T, W), BF16),
            jax.ShapeDtypeStruct((1, 1), F32),
            pltpu.VMEM((128, W), F32),
        ),
        in_specs=[anywhere] * 9,
        out_specs=(
            pl.BlockSpec(memory_space=pltpu.VMEM),
            pl.BlockSpec(memory_space=pltpu.SMEM),
            pl.BlockSpec(memory_space=pltpu.VMEM),
        ),
        scratch_shapes=scratch,
        compiler_params=pltpu.CompilerParams(
            collective_id=0, has_side_effects=True, vmem_limit_bytes=60 * 1024 * 1024
        ),
    )(
        tokens, w_latent.T, w_query, w_key_up, w_value_up, w_stu_query, w_stu_key, w_stu_value, forget.T
    )
    teacher, wgrad = pl.pallas_call(
        finish,
        out_shape=(jax.ShapeDtypeStruct((T, W), BF16), jax.ShapeDtypeStruct((128, W), F32)),
        in_specs=[pl.BlockSpec(memory_space=pltpu.VMEM)] * 2,
        out_specs=(anywhere, anywhere),
        scratch_shapes=[dma((2,))],
        compiler_params=pltpu.CompilerParams(vmem_limit_bytes=4 * 1024 * 1024),
    )(teacher, wgrad)
    return teacher, loss[0, 0], wgrad


def solution(mesh):
    return jax.shard_map(
        per_device,
        mesh=mesh,
        in_specs=(
            P("seq", None),
            P(None, "tensor"),
            P(None, "tensor"),
            P(None, "tensor"),
            P(None, "tensor"),
            P(None, "tensor"),
            P(None, "tensor"),
            P(None, "tensor"),
            P("seq", "tensor"),
        ),
        out_specs=(P("seq", "tensor"), P(), P("seq", "tensor")),
        check_vma=False,
    )
```

```python
import math

import jax
import jax.numpy as jnp
from jax import lax
from jax.experimental import pallas as pl
from jax.experimental.pallas import tpu as pltpu
from jax.sharding import PartitionSpec as P

F32 = jnp.float32
BF16 = jnp.bfloat16
MESH = pl.DeviceIdType.MESH
NEG_FILL = -1e30
EPSILON = 1e-06

T = 512
D = 2048
HD = 128
NH = 2
W = NH * HD
LAT = 512
HALF = T // 2
ONES = 16
NA = 32
ALL_TOKENS = 8192
ALL_HEADS = 16
EXP2_SCALE = math.log2(math.e) / math.sqrt(HD)

AWAY = (
    (-1, 0), (1, 0), (0, -1), (0, 1),
    (-1, -1), (1, -1), (2, 0), (0, 2), (-1, 1), (1, 1),
    (-1, 2), (1, 2), (2, -1), (2, 1),
    (2, 2),
)
LEVEL_OVER_Z = ((0, 1, 2, 3), (4, 5, 8, 9), (10, 11, 12, 13), (14,))
LEVEL_STEP = 4


def nt(a, b):
    return lax.dot_general(a, b, (((1,), (1,)), ((), ())), preferred_element_type=F32)


def nn(a, b):
    return jnp.dot(a, b, preferred_element_type=F32)


def tn(a, b):
    return lax.dot_general(a, b, (((0,), (0,)), ((), ())), preferred_element_type=F32)


def pick(index, values):
    out = jnp.int32(values[0])
    for k in range(1, len(values)):
        out = jnp.where(index == k, jnp.int32(values[k]), out)
    return out


def three_parts(a):
    hi = a.astype(BF16)
    rest = a - hi.astype(F32)
    mid = rest.astype(BF16)
    low = (rest - mid.astype(F32)).astype(BF16)
    return hi, mid, low


def kernel(
    tok_h, wl_h, wq_h, wku_h, wvu_h, wsq_h, wsk_h, wsv_h, fg_h,
    tout_ref, loss_ref, wg_ref,
    tok, tokt, wl, wall, wk, wv, wvt, fgv,
    lat, myp, pairin, pairbuf, kbuf, vt, qbuf, acc, mrun,
    sq, sk, sv, ccol, crow, mix, sout, startq, endk, vg,
    held, heldlog, sx, sy, mx, my, bx, by, lx, ly, lz, lc,
    pw, r1in, r1own, r2in, gw, gwin, hrow, lown, lin, a1in, a1own, a2in,
    load_sem, pair_s, pair_r, z_s, z_r, gs, gr, zg_s, zg_r, ds_, dr,
    st_s, st_r, rs_s, rs_r, ls_s, ls_r, gw_s, gw_r,
):
    s = lax.axis_index("seq")
    t = lax.axis_index("tensor")
    y, x = s // 4, s % 4
    z, c = t // 2, t % 2
    hb = c * HALF

    def plane(yy, xx):
        return (yy * 4 + xx, t)

    def x_peer(d):
        return plane(y, (x + d) % 4)

    def y_peer(d):
        return plane((y + d) % 4, x)

    def z_peer(d):
        return (s, ((z + d) % 4) * 2 + c)

    partner = (s, z * 2 + (1 - c))

    def remote(src, dst, send, recv, to):
        return pltpu.make_async_remote_copy(
            src_ref=src, dst_ref=dst, send_sem=send, recv_sem=recv, device_id=to, device_id_type=MESH
        )

    wl[...] = jnp.zeros_like(wl)
    loads = [
        pltpu.make_async_copy(wl_h, wl.at[pl.ds(pl.multiple_of(c * 64, 64), 64), :], load_sem.at[0]),
        pltpu.make_async_copy(tok_h, tok, load_sem.at[1]),
        pltpu.make_async_copy(wq_h, wall.at[0], load_sem.at[2]),
        pltpu.make_async_copy(wsk_h, wall.at[1], load_sem.at[3]),
        pltpu.make_async_copy(wsv_h, wall.at[2], load_sem.at[4]),
        pltpu.make_async_copy(wsq_h, wall.at[3], load_sem.at[5]),
        pltpu.make_async_copy(fg_h, fgv, load_sem.at[6]),
    ]
    for j in range(4):
        rows = pl.ds(pl.multiple_of((z + j) % 4 * HD, HD), HD)
        loads.append(pltpu.make_async_copy(wku_h.at[rows, :], wk.at[j * HD : (j + 1) * HD, :], load_sem.at[7 + j]))
        loads.append(pltpu.make_async_copy(wvu_h.at[rows, :], wv.at[j * HD : (j + 1) * HD, :], load_sem.at[11 + j]))
    loads[0].start()
    loads[1].start()
    barrier = pltpu.get_barrier_semaphore()
    peers = [x_peer(d) for d in (1, 2, 3)] + [y_peer(d) for d in (1, 2, 3)]
    peers += [z_peer(d) for d in (1, 2, 3)] + [partner]
    for peer in peers:
        pl.semaphore_signal(barrier, inc=1, device_id=peer, device_id_type=MESH)

    loads[0].wait()
    loads[1].wait()
    for copy in loads[2:]:
        copy.start()
    myp[...] = nt(tok[...], wl[...]).astype(BF16)
    pl.semaphore_wait(barrier, 10)
    other = pl.multiple_of((1 - c) * HALF, HALF)
    own = pl.multiple_of(hb, HALF)
    to_pair = remote(myp.at[pl.ds(other, HALF), :], pairin, pair_s, pair_r, partner)
    to_pair.start()

    def project(i):
        return nn(tok[...], wall[i])

    loads[2].wait()
    qbuf[...] = project(0).astype(BF16)
    to_pair.wait_recv()
    pairbuf[...] = myp[pl.ds(own, HALF), :] + pairin[...]
    my_slice = lat.at[y, x, z, pl.ds(own, HALF), :]
    lat[y, x, 0, pl.ds(own, HALF), :] = pairbuf[...]

    def slot(yy, xx, j):
        return lat.at[yy, xx, j, pl.ds(own, HALF), :]

    to_z = [
        remote(pairbuf, slot(y, x, 4 - d), z_s.at[d - 1], z_r.at[d - 1], z_peer(d)) for d in (1, 2, 3)
    ]
    for d in (3, 1, 2):
        to_z[d - 1].start()
    xp, xm, yp, ym = x_peer(1), x_peer(3), y_peer(1), y_peer(3)

    def near(j):
        return [
            remote(slot(y, x, j), slot(y, x, j), gs.at[32 + 2 * k + j], gr.at[32 + 2 * k + j], to)
            for k, to in enumerate((yp, ym, xp, xm))
        ]

    level_1 = [near(0), near(1)]
    for copy in level_1[0]:
        copy.start()

    def unit(h, m):
        part = m[:, h * HD : (h + 1) * HD]
        return part * lax.rsqrt(jnp.sum(part * part, axis=-1, keepdims=True) + EPSILON)

    loads[6].wait()
    row_at = lax.broadcasted_iota(jnp.int32, (T, T), 0)
    col_at = lax.broadcasted_iota(jnp.int32, (T, T), 1)
    lower = (col_at <= row_at).astype(BF16)
    f_parts = three_parts(fgv[...])
    crow[0:NH, :] = sum(nt(part, lower) for part in f_parts)
    for h in range(NH):
        spread = [jnp.broadcast_to(part[h : h + 1, :], (HD, T)) for part in f_parts]
        ccol[h] = sum(nt(lower, part) for part in spread)

    loads[3].wait()
    keys_f = project(1)
    loads[4].wait()
    sv[...] = project(2).astype(BF16)
    to_z[2].wait_recv()
    for copy in level_1[1]:
        copy.start()
    ends = []
    for h in range(NH):
        cols = slice(h * HD, (h + 1) * HD)
        unit_k = unit(h, keys_f)
        sk[:, cols] = unit_k.astype(BF16)
        end_row = ccol[h, T - 1 : T, :]
        endk[:, cols] = (unit_k * jnp.exp(end_row - ccol[h])).astype(BF16)
        ends.append(end_row)
    blank = jnp.zeros((8 - NH, HD), F32)
    mx[x] = jnp.concatenate(ends + [blank], axis=0)
    for h in range(NH):
        cols = slice(h * HD, (h + 1) * HD)
        sx[x, cols, :] = tn(endk[:, cols], sv[:, cols]).astype(BF16)

    def row_sends(buf, sems, first, peer_of, slot):
        return [
            remote(buf.at[slot], buf.at[slot], sems[0].at[first + d - 1], sems[1].at[first + d - 1], peer_of(d))
            for d in (2, 1, 3)
        ]

    st = (st_s, st_r)
    fwd_x = row_sends(sx, st, 0, x_peer, x)
    ends_x = row_sends(mx, st, 3, x_peer, x)
    for copy in ends_x:
        copy.start()
    loads[5].wait()
    queries_f = project(3)
    for h in range(NH):
        cols = slice(h * HD, (h + 1) * HD)
        unit_q = unit(h, queries_f)
        sq[:, cols] = unit_q.astype(BF16)
        startq[:, cols] = (unit_q * jnp.exp(ccol[h])).astype(BF16)

    def piece(idx, yy, xx, lo, size, to, slots=slice(0, 2)):
        ref = lat.at[yy % 4, xx % 4, slots, pl.ds(pl.multiple_of(hb + lo, 64), size), :]
        return remote(ref, ref, gs.at[idx], gr.at[idx], to)

    level_2 = [
        piece(4, y, x - 1, 0, 128, xp),
        piece(5, y, x + 1, 128, 128, xm),
        piece(6, y - 1, x, 0, 128, yp),
        piece(7, y + 1, x, 128, 128, ym),
        piece(8, y, x - 1, 0, 128, yp),
        piece(9, y, x - 1, 0, 128, ym),
        piece(10, y, x + 1, 0, 128, yp),
        piece(11, y, x + 1, 0, 128, ym),
        piece(12, y - 1, x, 128, 128, xp),
        piece(13, y - 1, x, 128, 128, xm),
        piece(14, y + 1, x, 128, 128, xp),
        piece(15, y + 1, x, 128, 128, xm),
    ]
    level_3 = [
        piece(16, y, x + 2, 0, 128, yp),
        piece(17, y, x + 2, 0, 128, ym),
        piece(18, y + 2, x, 128, 128, xp),
        piece(19, y + 2, x, 128, 128, xm),
        piece(20, y - 1, x - 1, 0, 64, yp),
        piece(21, y + 1, x - 1, 64, 64, ym),
        piece(22, y - 1, x + 1, 0, 64, yp),
        piece(23, y + 1, x + 1, 64, 64, ym),
        piece(24, y - 1, x - 1, 128, 64, xp),
        piece(25, y - 1, x + 1, 192, 64, xm),
        piece(26, y + 1, x - 1, 128, 64, xp),
        piece(27, y + 1, x + 1, 192, 64, xm),
    ]
    level_4 = [
        piece(28, y - 1, x + 2, 0, 64, yp),
        piece(29, y + 1, x + 2, 64, 64, ym),
        piece(30, y + 2, x - 1, 128, 64, xp),
        piece(31, y + 2, x + 1, 192, 64, xm),
    ]
    rest = slice(2, 4)
    rest_y = [piece(40, y - 1, x, 0, 128, yp, rest), piece(41, y + 1, x, 128, 128, ym, rest)]
    rest_x = [piece(42, y, x - 1, 0, 128, xp, rest), piece(43, y, x + 1, 128, 128, xm, rest)]
    levels = (sum(level_1, []), level_2, level_3, level_4)

    def to_partner(i, yy, xx):
        ref = lat.at[yy, xx, :, pl.ds(own, HALF), :]
        return remote(ref, ref, ds_.at[i], dr.at[i], partner)

    def other_slices(b, yy, xx):
        return (
            remote(slot(yy, xx, 0), slot(yy, xx, 3), zg_s.at[2 * b], zg_r.at[2 * b], z_peer(1)),
            remote(slot(yy, xx, 1), slot(yy, xx, 2), zg_s.at[2 * b + 1], zg_r.at[2 * b + 1], z_peer(3)),
        )

    def arrive(n):
        for copy in levels[n]:
            copy.wait_recv()
        if n < 3:
            for copy in levels[n + 1]:
                copy.start()
        for b in LEVEL_OVER_Z[n]:
            for copy in other_slices(b, *away(b)):
                copy.start()

    def away(i):
        return (y + AWAY[i][0]) % 4, (x + AWAY[i][1]) % 4

    to_z[0].wait_recv()
    to_z[1].wait_recv()
    own_to_partner = to_partner(15, y, x)
    own_to_partner.start()
    arrive(0)

    for h in range(NH):
        cols = slice(h * HD, (h + 1) * HD)
        raw = nt(sq[:, cols], sk[:, cols])
        gaps = ccol[h, :, 0:1] - crow[h : h + 1, :]
        mix[h] = (raw * jnp.exp(jnp.where(col_at <= row_at, gaps, NEG_FILL))).astype(BF16)
    for h in range(NH):
        cols = slice(h * HD, (h + 1) * HD)
        sout[:, cols] = nn(mix[h], sv[:, cols])

    def stage(buf, decays, position, order, h):
        rows = slice(h * HD, (h + 1) * HD)
        running = jnp.zeros((HD, HD), F32)
        total = jnp.zeros((1, HD), F32)
        inside, inside_log = running, total
        for k in order:
            here = position == k
            inside = jnp.where(here, running, inside)
            inside_log = jnp.where(here, total, inside_log)
            log_decay = decays[k, h : h + 1, :]
            running = running * jnp.exp(log_decay) + buf[k, rows, :].astype(F32)
            total = total + log_decay
        return inside, inside_log, running, total

    rise, fall = (0, 1, 2, 3), (3, 2, 1, 0)
    fwd_y = row_sends(sy, st, 6, y_peer, y) + row_sends(my, st, 9, y_peer, y)

    def forward_row():
        for copy in fwd_x:
            copy.wait_recv()
        ends = []
        for h in range(NH):
            rows = slice(h * HD, (h + 1) * HD)
            inside, inside_log, running, total = stage(sx, mx, x, rise, h)
            held[rows, :] = inside
            heldlog[h : h + 1, :] = inside_log
            sy[y, rows, :] = running.astype(BF16)
            ends.append(total)
        my[y] = jnp.concatenate(ends + [blank], axis=0)
        for copy in fwd_y:
            copy.start()

    def tok_turn(i, carry):
        cut = pl.ds(pl.multiple_of(i * 256, 256), 256)
        tokt[cut, :] = jnp.transpose(tok[:, cut])
        return carry

    lax.fori_loop(0, D // 256, tok_turn, 0)

    for copy in loads[7:]:
        copy.wait()
    wvt[...] = jnp.transpose(wv[...])
    for h in range(NH):
        vt[h, HD:, :] = jnp.ones((ONES, 2 * T), BF16)

    def attend(blocks, masked=False):
        keys = T * len(blocks)
        arrays = []
        for n, (yy, xx) in enumerate(blocks):
            block = jnp.concatenate([lat[yy, xx, k] for k in range(4)], axis=1)
            kbuf[n * T : (n + 1) * T, :] = nn(block, wk[...]).astype(BF16)
            arrays.append(block)
        scores = [
            nt(kbuf[0:keys, h * HD : (h + 1) * HD], qbuf[:, h * HD : (h + 1) * HD]) for h in range(NH)
        ]
        for n, block in enumerate(arrays):
            values = nt(wvt[...], block).astype(BF16)
            for h in range(NH):
                vt[h, 0:HD, n * T : (n + 1) * T] = values[h * HD : (h + 1) * HD, :]
        for h in range(NH):
            score = scores[h]
            if masked:
                score = jnp.where(row_at <= col_at, score, NEG_FILL)
            best = jnp.max(score, axis=0, keepdims=True)
            if not masked:
                old = mrun[h : h + 1, :]
                best = jnp.maximum(old, best)
            weights = jnp.exp2((score - best) * EXP2_SCALE).astype(BF16)
            part = nn(vt[h, :, 0:keys], weights)
            if not masked:
                part += acc[h] * jnp.exp2((old - best) * EXP2_SCALE)
            acc[h] = part
            mrun[h : h + 1, :] = best

    own_to_partner.wait_recv()
    attend([(y, x)], masked=True)

    def place(b):
        yy = (y + pick(b, [a[0] for a in AWAY]) + 4) % 4
        xx = (x + pick(b, [a[1] for a in AWAY]) + 4) % 4
        return yy, xx

    def pass_on(b):
        yy, xx = place(b)
        for copy in other_slices(b, yy, xx):
            copy.wait_recv()
        to_partner(b, yy, xx).start()

    for copy in ends_x:
        copy.wait_recv()
    for h in range(NH):
        cols = slice(h * HD, (h + 1) * HD)
        to_end = sum(jnp.where(x < k, mx[k, h : h + 1, :], 0.0) for k in (1, 2, 3))
        faded = (endk[:, cols].astype(F32) * jnp.exp(to_end)).astype(BF16)
        for i in range(4):
            part = nn(tokt[i * 512 : (i + 1) * 512, :], faded).astype(BF16)
            for k in range(4):
                gw[h, i, k] = part[k * 128 : (k + 1) * 128, :]
    row_gw = [
        [
            remote(gw.at[h, :, (x + d) % 4], gwin.at[h, d - 1], gw_s.at[3 * h + d - 1], gw_r.at[3 * h + d - 1], x_peer(d))
            for d in (2, 1, 3)
        ]
        for h in range(NH)
    ]
    arrive(1)
    for copy in fwd_x:
        copy.start()
    pass_on(0)
    pass_on(1)
    for copy in rest_y:
        copy.start()

    def block_step(i, carry):
        @pl.when(i == LEVEL_STEP)
        def _():
            arrive(3)
            forward_row()

        for h, step in ((0, 3), (1, 4)):

            @pl.when(i == step)
            def _():
                for copy in row_gw[h]:
                    copy.start()

        ahead = jnp.logical_or(i == 0, i >= 3)

        @pl.when(jnp.logical_and(i < 7, ahead))
        def _():
            pass_on(2 * i + 2)

        @pl.when(jnp.logical_and(i < 6, ahead))
        def _():
            pass_on(2 * i + 3)

        @pl.when(i == 0)
        def _():
            for copy in rest_x:
                copy.start()

        @pl.when(i == 2)
        def _():
            for b, copies in ((6, rest_y), (7, rest_x)):
                for copy in copies:
                    copy.wait_recv()
                to_partner(b, *away(b)).start()

        y1, x1 = place(2 * i)
        to_partner(2 * i, y1, x1).wait_recv()
        y2, x2 = place(2 * i + 1)

        @pl.when(i < 7)
        def _():
            to_partner(2 * i + 1, y2, x2).wait_recv()

        need_1 = y1 * 4 + x1 < s
        need_2 = jnp.logical_and(y2 * 4 + x2 < s, i < 7)

        @pl.when(jnp.logical_and(need_1, need_2))
        def _():
            attend([(y1, x1), (y2, x2)])

        @pl.when(need_1 != need_2)
        def _():
            attend([(jnp.where(need_1, y1, y2), jnp.where(need_1, x1, x2))])

        @pl.when(i == 1)
        def _():
            arrive(2)
            pass_on(4)
            pass_on(5)

        return carry

    lax.fori_loop(0, 8, block_step, 0)

    for copy in fwd_y:
        copy.wait_recv()
    for h in range(NH):
        cols = slice(h * HD, (h + 1) * HD)
        inside_y = stage(sy, my, y, rise, h)[0]
        prefix = (held[cols, :] + jnp.exp(heldlog[h : h + 1, :]) * inside_y).astype(BF16)
        sout[:, cols] = sout[:, cols] + nn(startq[:, cols], prefix)

    def head_sends(buf, first, peer_of, slot, h):
        ref = buf.at[slot, h * HD : (h + 1) * HD, :]
        at = [first + 3 * h + d - 1 for d in (2, 1, 3)]
        return [remote(ref, ref, st_s.at[k], st_r.at[k], peer_of(d)) for k, d in zip(at, (2, 1, 3))]

    back_x = [head_sends(bx, 12, x_peer, x, h) for h in range(NH)]
    back_y = [head_sends(by, 18, y_peer, y, h) for h in range(NH)]
    squares = jnp.zeros((8, HD), F32)
    inv = 1.0 / math.sqrt(ALL_TOKENS)
    for h in range(NH):
        cols = slice(h * HD, (h + 1) * HD)
        teacher = jnp.transpose(acc[h, 0:HD, :] / acc[h, HD : HD + 1, :]).astype(BF16)
        tout_ref[:, cols] = teacher
        mismatch = sout[:, cols] - teacher.astype(F32)
        squares += jnp.sum((mismatch * mismatch).reshape(T // 8, 8, HD), axis=0)
        vg[:, cols] = (mismatch * inv).astype(BF16)
        bx[x, cols, :] = tn(startq[:, cols], vg[:, cols]).astype(BF16)
        for copy in back_x[h]:
            copy.start()
    lx[x] = squares
    ls = (ls_s, ls_r)
    loss_x = row_sends(lx, ls, 0, x_peer, x)
    for copy in loss_x:
        copy.start()
    for h in range(NH):
        cols = slice(h * HD, (h + 1) * HD)
        sout[:, cols] = tn(mix[h], vg[:, cols])

    row_inside = []
    for h in range(NH):
        for copy in back_x[h]:
            copy.wait_recv()
        inside, inside_log, running, _ = stage(bx, mx, x, fall, h)
        row_inside.append(inside.astype(BF16))
        by[y, h * HD : (h + 1) * HD, :] = running.astype(BF16)
        for copy in back_y[h]:
            copy.start()
    for copy in loss_x:
        copy.wait_recv()
    ly[y] = lx[0] + lx[1] + lx[2] + lx[3]
    loss_y = row_sends(ly, ls, 3, y_peer, y)
    for copy in loss_y:
        copy.start()

    def value_gradient(h):
        cols = slice(h * HD, (h + 1) * HD)
        vg[:, cols] = (sout[:, cols] + nn(endk[:, cols], row_inside[h])).astype(BF16)

    def from_later_rows(h):
        for copy in back_y[h]:
            copy.wait_recv()
        return nn(hrow[h], stage(by, my, y, fall, h)[0].astype(BF16))

    def weight_gradient(h):
        values = vg[:, h * HD : (h + 1) * HD]
        for i in range(4):
            part = nn(tokt[i * 512 : (i + 1) * 512, :], values).astype(BF16)
            for k in range(4):
                pw[h, i, k] = part[k * 128 : (k + 1) * 128, :]

    rs_x1 = [
        remote(pw.at[0, :, (x + d) % 4], r1in.at[0, d - 1], rs_s.at[d - 1], rs_r.at[d - 1], x_peer(d))
        for d in (2, 1, 3)
    ]
    rs_y1 = [
        remote(
            pw.at[1, (y + d) % 4, :, NA:, :],
            r1in.at[1, d - 1, :, NA:, :],
            rs_s.at[d + 2],
            rs_r.at[d + 2],
            y_peer(d),
        )
        for d in (1, 3, 2)
    ]
    rs_a1 = [
        remote(pw.at[1, :, (x + d) % 4, 0:NA, :], a1in.at[d - 1], rs_s.at[d + 14], rs_r.at[d + 14], x_peer(d))
        for d in (2, 1, 3)
    ]
    value_gradient(0)
    value_gradient(1)
    weight_gradient(1)
    for copy in rs_y1 + rs_a1:
        copy.start()
    weight_gradient(0)
    for copy in rs_x1:
        copy.start()
    for h in range(NH):
        for copy in row_gw[h]:
            copy.wait_recv()
        for k in range(4):
            total = gw[h, k, x].astype(F32) + sum(gwin[h, d, k].astype(F32) for d in range(3))
            hrow[h, k * 128 : (k + 1) * 128, :] = total.astype(BF16)
    later = from_later_rows(0)
    later_1 = from_later_rows(1)
    for k in range(4):
        lown[k] = later_1[k * 128 + NA : (k + 1) * 128, :].astype(BF16)
    rows_y = [
        remote(lown.at[(y + d) % 4], lin.at[d - 1], rs_s.at[d + 11], rs_r.at[d + 11], y_peer(d)) for d in (2, 1, 3)
    ]
    for copy in rows_y:
        copy.start()
    for copy in loss_y:
        copy.wait_recv()
    lz[z] = ly[0] + ly[1] + ly[2] + ly[3]
    loss_z = row_sends(lz, ls, 6, z_peer, z)
    for copy in loss_z:
        copy.start()

    for copy in rs_x1:
        copy.wait_recv()
    mine = [pw[0, k, x].astype(F32) for k in range(4)]
    for k in range(4):
        total = mine[k] + later[k * 128 : (k + 1) * 128, :]
        r1own[0, k] = (total + sum(r1in[0, d, k].astype(F32) for d in range(3))).astype(BF16)
    rs_y2 = [
        remote(r1own.at[0, (y + d) % 4], r2in.at[0, d - 1], rs_s.at[d + 5], rs_r.at[d + 5], y_peer(d))
        for d in (2, 1, 3)
    ]
    for copy in rs_y2:
        copy.start()
    for copy in rs_a1:
        copy.wait_recv()
    for k in range(4):
        total = pw[1, k, x, 0:NA, :].astype(F32) + later_1[k * 128 : k * 128 + NA, :]
        a1own[k] = (total + sum(a1in[d, k].astype(F32) for d in range(3))).astype(BF16)
    rs_a2 = [
        remote(a1own.at[(y + d) % 4], a2in.at[d - 1], rs_s.at[d + 17], rs_r.at[d + 17], y_peer(d)) for d in (2, 1, 3)
    ]
    for copy in rs_a2:
        copy.start()
    for copy in rs_y1:
        copy.wait_recv()
    mine = [pw[1, y, k, NA:, :].astype(F32) for k in range(4)]
    for k in range(4):
        total = mine[k] + sum(r1in[1, d, k, NA:, :].astype(F32) for d in range(3))
        r1own[1, k, NA:, :] = total.astype(BF16)
    rs_x2 = [
        remote(
            r1own.at[1, (x + d) % 4, NA:, :],
            r2in.at[1, d - 1, NA:, :],
            rs_s.at[d + 8],
            rs_r.at[d + 8],
            x_peer(d),
        )
        for d in (2, 1, 3)
    ]
    for copy in rs_x2:
        copy.start()

    for copy in loss_z:
        copy.wait_recv()
    lc[c] = lz[0] + lz[1] + lz[2] + lz[3]
    loss_c = remote(lc.at[c], lc.at[c], ls_s.at[9], ls_r.at[9], partner)
    loss_c.start()
    loss_c.wait_recv()
    loss_ref[0, 0] = jnp.sum(lc[0] + lc[1]) / (2.0 * ALL_TOKENS * ALL_HEADS * HD)

    for copy in rs_y2:
        copy.wait_recv()
    wg_ref[:, 0:HD] = r1own[0, y].astype(F32) + sum(r2in[0, d].astype(F32) for d in range(3))
    for copy in rows_y:
        copy.wait_recv()
    late = lown[y].astype(F32) + sum(lin[d].astype(F32) for d in range(3))
    for copy in rs_x2:
        copy.wait_recv()
    partial = r1own[1, x, NA:, :].astype(F32) + sum(r2in[1, d, NA:, :].astype(F32) for d in range(3))
    wg_ref[NA:, HD:W] = late + partial
    for copy in rs_a2:
        copy.wait_recv()
    wg_ref[0:NA, HD:W] = a1own[y].astype(F32) + sum(a2in[d].astype(F32) for d in range(3))

    sent = [to_pair] + to_z + fwd_x + fwd_y + sum(back_x + back_y, [])
    sent += loss_x + loss_y + loss_z + [loss_c] + rs_x1 + rs_y1 + rs_y2 + rs_x2
    sent += rs_a1 + rs_a2 + ends_x + sum(row_gw, []) + rows_y
    for level in levels:
        sent += level
    for b in range(15):
        sent += [to_partner(b, *away(b))]
    for blocks in LEVEL_OVER_Z:
        for b in blocks:
            sent += other_slices(b, *away(b))
    sent += rest_x + rest_y
    sent.append(own_to_partner)
    for copy in sent:
        copy.wait_send()


def finish(teacher_ref, wgrad_ref, teacher_out, wgrad_out, sem):
    copies = [
        pltpu.make_async_copy(teacher_ref, teacher_out, sem.at[0]),
        pltpu.make_async_copy(wgrad_ref, wgrad_out, sem.at[1]),
    ]
    for copy in copies:
        copy.start()
    for copy in copies:
        copy.wait()


def per_device(tokens, w_latent, w_query, w_key_up, w_value_up, w_stu_query, w_stu_key, w_stu_value, forget):
    dma = pltpu.SemaphoreType.DMA
    scratch = [
        pltpu.VMEM((T, D), BF16),
        pltpu.VMEM((D, T), BF16),
        pltpu.VMEM((HD, D), BF16),
        pltpu.VMEM((4, D, W), BF16),
        pltpu.VMEM((LAT, W), BF16),
        pltpu.VMEM((LAT, W), BF16),
        pltpu.VMEM((W, LAT), BF16),
        pltpu.VMEM((NH, T), F32),
        pltpu.VMEM((4, 4, 4, T, HD), BF16),
        pltpu.VMEM((T, HD), BF16),
        pltpu.VMEM((HALF, HD), BF16),
        pltpu.VMEM((HALF, HD), BF16),
        pltpu.VMEM((2 * T, W), BF16),
        pltpu.VMEM((NH, HD + ONES, 2 * T), BF16),
        pltpu.VMEM((T, W), BF16),
        pltpu.VMEM((NH, HD + ONES, T), F32),
        pltpu.VMEM((8, T), F32),
        pltpu.VMEM((T, W), BF16),
        pltpu.VMEM((T, W), BF16),
        pltpu.VMEM((T, W), BF16),
        pltpu.VMEM((NH, T, HD), F32),
        pltpu.VMEM((8, T), F32),
        pltpu.VMEM((NH, T, T), BF16),
        pltpu.VMEM((T, W), F32),
        pltpu.VMEM((T, W), BF16),
        pltpu.VMEM((T, W), BF16),
        pltpu.VMEM((T, W), BF16),
        pltpu.VMEM((W, HD), F32),
        pltpu.VMEM((8, HD), F32),
        pltpu.VMEM((4, W, HD), BF16),
        pltpu.VMEM((4, W, HD), BF16),
        pltpu.VMEM((4, 8, HD), F32),
        pltpu.VMEM((4, 8, HD), F32),
        pltpu.VMEM((4, W, HD), BF16),
        pltpu.VMEM((4, W, HD), BF16),
        pltpu.VMEM((4, 8, HD), F32),
        pltpu.VMEM((4, 8, HD), F32),
        pltpu.VMEM((4, 8, HD), F32),
        pltpu.VMEM((2, 8, HD), F32),
        pltpu.VMEM((NH, 4, 4, 128, HD), BF16),
        pltpu.VMEM((NH, 3, 4, 128, HD), BF16),
        pltpu.VMEM((NH, 4, 128, HD), BF16),
        pltpu.VMEM((NH, 3, 128, HD), BF16),
        pltpu.VMEM((NH, 4, 4, 128, HD), BF16),
        pltpu.VMEM((NH, 3, 4, 128, HD), BF16),
        pltpu.VMEM((NH, 512, HD), BF16),
        pltpu.VMEM((4, 128 - NA, HD), BF16),
        pltpu.VMEM((3, 128 - NA, HD), BF16),
        pltpu.VMEM((3, 4, NA, HD), BF16),
        pltpu.VMEM((4, NA, HD), BF16),
        pltpu.VMEM((3, NA, HD), BF16),
        dma((15,)),
        dma,
        dma,
        dma((3,)),
        dma((3,)),
        dma((44,)),
        dma((44,)),
        dma((30,)),
        dma((30,)),
        dma((16,)),
        dma((16,)),
        dma((24,)),
        dma((24,)),
        dma((21,)),
        dma((21,)),
        dma((10,)),
        dma((10,)),
        dma((6,)),
        dma((6,)),
    ]
    anywhere = pl.BlockSpec(memory_space=pl.ANY)
    teacher, loss, wgrad = pl.pallas_call(
        kernel,
        out_shape=(
            pltpu.VMEM((T, W), BF16),
            jax.ShapeDtypeStruct((1, 1), F32),
            pltpu.VMEM((128, W), F32),
        ),
        in_specs=[anywhere] * 9,
        out_specs=(
            pl.BlockSpec(memory_space=pltpu.VMEM),
            pl.BlockSpec(memory_space=pltpu.SMEM),
            pl.BlockSpec(memory_space=pltpu.VMEM),
        ),
        scratch_shapes=scratch,
        compiler_params=pltpu.CompilerParams(
            collective_id=0, has_side_effects=True, vmem_limit_bytes=60 * 1024 * 1024
        ),
    )(
        tokens, w_latent.T, w_query, w_key_up, w_value_up, w_stu_query, w_stu_key, w_stu_value, forget.T
    )
    teacher, wgrad = pl.pallas_call(
        finish,
        out_shape=(jax.ShapeDtypeStruct((T, W), BF16), jax.ShapeDtypeStruct((128, W), F32)),
        in_specs=[pl.BlockSpec(memory_space=pltpu.VMEM)] * 2,
        out_specs=(anywhere, anywhere),
        scratch_shapes=[dma((2,))],
        compiler_params=pltpu.CompilerParams(vmem_limit_bytes=4 * 1024 * 1024),
    )(teacher, wgrad)
    return teacher, loss[0, 0], wgrad


def solution(mesh):
    return jax.shard_map(
        per_device,
        mesh=mesh,
        in_specs=(
            P("seq", None),
            P(None, "tensor"),
            P(None, "tensor"),
            P(None, "tensor"),
            P(None, "tensor"),
            P(None, "tensor"),
            P(None, "tensor"),
            P(None, "tensor"),
            P("seq", "tensor"),
        ),
        out_specs=(P("seq", "tensor"), P(), P("seq", "tensor")),
        check_vma=False,
    )
```

```python
import math

import jax
import jax.numpy as jnp
from jax import lax
from jax.experimental import pallas as pl
from jax.experimental.pallas import tpu as pltpu
from jax.sharding import PartitionSpec as P

F32 = jnp.float32
BF16 = jnp.bfloat16
MESH = pl.DeviceIdType.MESH
NEG_FILL = -1e30
EPSILON = 1e-06

T = 512
D = 2048
HD = 128
NH = 2
W = NH * HD
LAT = 512
HALF = T // 2
ONES = 16
NA = 16
ALL_TOKENS = 8192
ALL_HEADS = 16
EXP2_SCALE = math.log2(math.e) / math.sqrt(HD)

AWAY = (
    (-1, 0), (1, 0), (0, -1), (0, 1),
    (-1, -1), (1, -1), (2, 0), (0, 2), (-1, 1), (1, 1),
    (-1, 2), (1, 2), (2, -1), (2, 1),
    (2, 2),
)
LEVEL_OVER_Z = ((0, 1, 2, 3), (4, 5, 8, 9), (10, 11, 12, 13), (14,))
LEVEL_STEP = 4


def nt(a, b):
    return lax.dot_general(a, b, (((1,), (1,)), ((), ())), preferred_element_type=F32)


def nn(a, b):
    return jnp.dot(a, b, preferred_element_type=F32)


def tn(a, b):
    return lax.dot_general(a, b, (((0,), (0,)), ((), ())), preferred_element_type=F32)


def pick(index, values):
    out = jnp.int32(values[0])
    for k in range(1, len(values)):
        out = jnp.where(index == k, jnp.int32(values[k]), out)
    return out


def three_parts(a):
    hi = a.astype(BF16)
    rest = a - hi.astype(F32)
    mid = rest.astype(BF16)
    low = (rest - mid.astype(F32)).astype(BF16)
    return hi, mid, low


def kernel(
    tok_h, wl_h, wq_h, wku_h, wvu_h, wsq_h, wsk_h, wsv_h, fg_h,
    tout_ref, loss_ref, wg_ref,
    tok, tokt, wl, wall, wk, wv, wvt, fgv,
    lat, myp, pairin, pairbuf, kbuf, vt, qbuf, acc, mrun,
    sq, sk, sv, ccol, crow, mix, sout, startq, endk, vg,
    held, heldlog, sx, sy, mx, my, bx, by, lx, ly, lz, lc,
    pw, r1in, r1own, r2in, gw, gwin, hrow, lown, lin, a1in, a1own, a2in,
    load_sem, pair_s, pair_r, z_s, z_r, gs, gr, zg_s, zg_r, ds_, dr,
    st_s, st_r, rs_s, rs_r, ls_s, ls_r, gw_s, gw_r,
):
    s = lax.axis_index("seq")
    t = lax.axis_index("tensor")
    y, x = s // 4, s % 4
    z, c = t // 2, t % 2
    hb = c * HALF

    def plane(yy, xx):
        return (yy * 4 + xx, t)

    def x_peer(d):
        return plane(y, (x + d) % 4)

    def y_peer(d):
        return plane((y + d) % 4, x)

    def z_peer(d):
        return (s, ((z + d) % 4) * 2 + c)

    partner = (s, z * 2 + (1 - c))

    def remote(src, dst, send, recv, to):
        return pltpu.make_async_remote_copy(
            src_ref=src, dst_ref=dst, send_sem=send, recv_sem=recv, device_id=to, device_id_type=MESH
        )

    wl[...] = jnp.zeros_like(wl)
    loads = [
        pltpu.make_async_copy(wl_h, wl.at[pl.ds(pl.multiple_of(c * 64, 64), 64), :], load_sem.at[0]),
        pltpu.make_async_copy(tok_h, tok, load_sem.at[1]),
        pltpu.make_async_copy(wq_h, wall.at[0], load_sem.at[2]),
        pltpu.make_async_copy(wsk_h, wall.at[1], load_sem.at[3]),
        pltpu.make_async_copy(wsv_h, wall.at[2], load_sem.at[4]),
        pltpu.make_async_copy(wsq_h, wall.at[3], load_sem.at[5]),
        pltpu.make_async_copy(fg_h, fgv, load_sem.at[6]),
    ]
    for j in range(4):
        rows = pl.ds(pl.multiple_of((z + j) % 4 * HD, HD), HD)
        loads.append(pltpu.make_async_copy(wku_h.at[rows, :], wk.at[j * HD : (j + 1) * HD, :], load_sem.at[7 + j]))
        loads.append(pltpu.make_async_copy(wvu_h.at[rows, :], wv.at[j * HD : (j + 1) * HD, :], load_sem.at[11 + j]))
    loads[0].start()
    loads[1].start()
    barrier = pltpu.get_barrier_semaphore()
    peers = [x_peer(d) for d in (1, 2, 3)] + [y_peer(d) for d in (1, 2, 3)]
    peers += [z_peer(d) for d in (1, 2, 3)] + [partner]
    for peer in peers:
        pl.semaphore_signal(barrier, inc=1, device_id=peer, device_id_type=MESH)

    loads[0].wait()
    loads[1].wait()
    for copy in loads[2:]:
        copy.start()
    myp[...] = nt(tok[...], wl[...]).astype(BF16)
    pl.semaphore_wait(barrier, 10)
    other = pl.multiple_of((1 - c) * HALF, HALF)
    own = pl.multiple_of(hb, HALF)
    to_pair = remote(myp.at[pl.ds(other, HALF), :], pairin, pair_s, pair_r, partner)
    to_pair.start()

    def project(i):
        return nn(tok[...], wall[i])

    loads[2].wait()
    qbuf[...] = project(0).astype(BF16)
    to_pair.wait_recv()
    pairbuf[...] = myp[pl.ds(own, HALF), :] + pairin[...]
    my_slice = lat.at[y, x, z, pl.ds(own, HALF), :]
    lat[y, x, 0, pl.ds(own, HALF), :] = pairbuf[...]

    def slot(yy, xx, j):
        return lat.at[yy, xx, j, pl.ds(own, HALF), :]

    to_z = [
        remote(pairbuf, slot(y, x, 4 - d), z_s.at[d - 1], z_r.at[d - 1], z_peer(d)) for d in (1, 2, 3)
    ]
    for d in (3, 1, 2):
        to_z[d - 1].start()
    xp, xm, yp, ym = x_peer(1), x_peer(3), y_peer(1), y_peer(3)

    def near(j):
        return [
            remote(slot(y, x, j), slot(y, x, j), gs.at[32 + 2 * k + j], gr.at[32 + 2 * k + j], to)
            for k, to in enumerate((yp, ym, xp, xm))
        ]

    level_1 = [near(0), near(1)]
    for copy in level_1[0]:
        copy.start()

    def unit(h, m):
        part = m[:, h * HD : (h + 1) * HD]
        return part * lax.rsqrt(jnp.sum(part * part, axis=-1, keepdims=True) + EPSILON)

    loads[6].wait()
    row_at = lax.broadcasted_iota(jnp.int32, (T, T), 0)
    col_at = lax.broadcasted_iota(jnp.int32, (T, T), 1)
    lower = (col_at <= row_at).astype(BF16)
    f_parts = three_parts(fgv[...])
    crow[0:NH, :] = sum(nt(part, lower) for part in f_parts)
    for h in range(NH):
        spread = [jnp.broadcast_to(part[h : h + 1, :], (HD, T)) for part in f_parts]
        ccol[h] = sum(nt(lower, part) for part in spread)

    loads[3].wait()
    keys_f = project(1)
    loads[4].wait()
    sv[...] = project(2).astype(BF16)
    to_z[2].wait_recv()
    for copy in level_1[1]:
        copy.start()
    ends = []
    for h in range(NH):
        cols = slice(h * HD, (h + 1) * HD)
        unit_k = unit(h, keys_f)
        sk[:, cols] = unit_k.astype(BF16)
        end_row = ccol[h, T - 1 : T, :]
        endk[:, cols] = (unit_k * jnp.exp(end_row - ccol[h])).astype(BF16)
        ends.append(end_row)
    blank = jnp.zeros((8 - NH, HD), F32)
    mx[x] = jnp.concatenate(ends + [blank], axis=0)
    for h in range(NH):
        cols = slice(h * HD, (h + 1) * HD)
        sx[x, cols, :] = tn(endk[:, cols], sv[:, cols]).astype(BF16)

    def row_sends(buf, sems, first, peer_of, slot):
        return [
            remote(buf.at[slot], buf.at[slot], sems[0].at[first + d - 1], sems[1].at[first + d - 1], peer_of(d))
            for d in (2, 1, 3)
        ]

    st = (st_s, st_r)
    fwd_x = row_sends(sx, st, 0, x_peer, x)
    ends_x = row_sends(mx, st, 3, x_peer, x)
    for copy in ends_x:
        copy.start()
    loads[5].wait()
    queries_f = project(3)
    for h in range(NH):
        cols = slice(h * HD, (h + 1) * HD)
        unit_q = unit(h, queries_f)
        sq[:, cols] = unit_q.astype(BF16)
        startq[:, cols] = (unit_q * jnp.exp(ccol[h])).astype(BF16)

    def piece(idx, yy, xx, lo, size, to, slots=slice(0, 2)):
        ref = lat.at[yy % 4, xx % 4, slots, pl.ds(pl.multiple_of(hb + lo, 64), size), :]
        return remote(ref, ref, gs.at[idx], gr.at[idx], to)

    level_2 = [
        piece(4, y, x - 1, 0, 128, xp),
        piece(5, y, x + 1, 128, 128, xm),
        piece(6, y - 1, x, 0, 128, yp),
        piece(7, y + 1, x, 128, 128, ym),
        piece(8, y, x - 1, 0, 128, yp),
        piece(9, y, x - 1, 0, 128, ym),
        piece(10, y, x + 1, 0, 128, yp),
        piece(11, y, x + 1, 0, 128, ym),
        piece(12, y - 1, x, 128, 128, xp),
        piece(13, y - 1, x, 128, 128, xm),
        piece(14, y + 1, x, 128, 128, xp),
        piece(15, y + 1, x, 128, 128, xm),
    ]
    level_3 = [
        piece(16, y, x + 2, 0, 128, yp),
        piece(17, y, x + 2, 0, 128, ym),
        piece(18, y + 2, x, 128, 128, xp),
        piece(19, y + 2, x, 128, 128, xm),
        piece(20, y - 1, x - 1, 0, 64, yp),
        piece(21, y + 1, x - 1, 64, 64, ym),
        piece(22, y - 1, x + 1, 0, 64, yp),
        piece(23, y + 1, x + 1, 64, 64, ym),
        piece(24, y - 1, x - 1, 128, 64, xp),
        piece(25, y - 1, x + 1, 192, 64, xm),
        piece(26, y + 1, x - 1, 128, 64, xp),
        piece(27, y + 1, x + 1, 192, 64, xm),
    ]
    level_4 = [
        piece(28, y - 1, x + 2, 0, 64, yp),
        piece(29, y + 1, x + 2, 64, 64, ym),
        piece(30, y + 2, x - 1, 128, 64, xp),
        piece(31, y + 2, x + 1, 192, 64, xm),
    ]
    rest = slice(2, 4)
    rest_y = [piece(40, y - 1, x, 0, 128, yp, rest), piece(41, y + 1, x, 128, 128, ym, rest)]
    rest_x = [piece(42, y, x - 1, 0, 128, xp, rest), piece(43, y, x + 1, 128, 128, xm, rest)]
    levels = (sum(level_1, []), level_2, level_3, level_4)

    def to_partner(i, yy, xx):
        ref = lat.at[yy, xx, :, pl.ds(own, HALF), :]
        return remote(ref, ref, ds_.at[i], dr.at[i], partner)

    def other_slices(b, yy, xx):
        return (
            remote(slot(yy, xx, 0), slot(yy, xx, 3), zg_s.at[2 * b], zg_r.at[2 * b], z_peer(1)),
            remote(slot(yy, xx, 1), slot(yy, xx, 2), zg_s.at[2 * b + 1], zg_r.at[2 * b + 1], z_peer(3)),
        )

    def arrive(n):
        for copy in levels[n]:
            copy.wait_recv()
        if n < 3:
            for copy in levels[n + 1]:
                copy.start()
        for b in LEVEL_OVER_Z[n]:
            for copy in other_slices(b, *away(b)):
                copy.start()

    def away(i):
        return (y + AWAY[i][0]) % 4, (x + AWAY[i][1]) % 4

    to_z[0].wait_recv()
    to_z[1].wait_recv()
    own_to_partner = to_partner(15, y, x)
    own_to_partner.start()
    arrive(0)

    for h in range(NH):
        cols = slice(h * HD, (h + 1) * HD)
        raw = nt(sq[:, cols], sk[:, cols])
        gaps = ccol[h, :, 0:1] - crow[h : h + 1, :]
        mix[h] = (raw * jnp.exp(jnp.where(col_at <= row_at, gaps, NEG_FILL))).astype(BF16)
    for h in range(NH):
        cols = slice(h * HD, (h + 1) * HD)
        sout[:, cols] = nn(mix[h], sv[:, cols])

    def stage(buf, decays, position, order, h):
        rows = slice(h * HD, (h + 1) * HD)
        running = jnp.zeros((HD, HD), F32)
        total = jnp.zeros((1, HD), F32)
        inside, inside_log = running, total
        for k in order:
            here = position == k
            inside = jnp.where(here, running, inside)
            inside_log = jnp.where(here, total, inside_log)
            log_decay = decays[k, h : h + 1, :]
            running = running * jnp.exp(log_decay) + buf[k, rows, :].astype(F32)
            total = total + log_decay
        return inside, inside_log, running, total

    rise, fall = (0, 1, 2, 3), (3, 2, 1, 0)
    fwd_y = row_sends(sy, st, 6, y_peer, y) + row_sends(my, st, 9, y_peer, y)

    def forward_row():
        for copy in fwd_x:
            copy.wait_recv()
        ends = []
        for h in range(NH):
            rows = slice(h * HD, (h + 1) * HD)
            inside, inside_log, running, total = stage(sx, mx, x, rise, h)
            held[rows, :] = inside
            heldlog[h : h + 1, :] = inside_log
            sy[y, rows, :] = running.astype(BF16)
            ends.append(total)
        my[y] = jnp.concatenate(ends + [blank], axis=0)
        for copy in fwd_y:
            copy.start()

    def tok_turn(i, carry):
        cut = pl.ds(pl.multiple_of(i * 256, 256), 256)
        tokt[cut, :] = jnp.transpose(tok[:, cut])
        return carry

    lax.fori_loop(0, D // 256, tok_turn, 0)

    for copy in loads[7:]:
        copy.wait()
    wvt[...] = jnp.transpose(wv[...])
    for h in range(NH):
        vt[h, HD:, :] = jnp.ones((ONES, 2 * T), BF16)

    def attend(blocks, masked=False):
        keys = T * len(blocks)
        arrays = []
        for n, (yy, xx) in enumerate(blocks):
            block = jnp.concatenate([lat[yy, xx, k] for k in range(4)], axis=1)
            kbuf[n * T : (n + 1) * T, :] = nn(block, wk[...]).astype(BF16)
            arrays.append(block)
        scores = [
            nt(kbuf[0:keys, h * HD : (h + 1) * HD], qbuf[:, h * HD : (h + 1) * HD]) for h in range(NH)
        ]
        for n, block in enumerate(arrays):
            values = nt(wvt[...], block).astype(BF16)
            for h in range(NH):
                vt[h, 0:HD, n * T : (n + 1) * T] = values[h * HD : (h + 1) * HD, :]
        for h in range(NH):
            score = scores[h]
            if masked:
                score = jnp.where(row_at <= col_at, score, NEG_FILL)
            best = jnp.max(score, axis=0, keepdims=True)
            if not masked:
                old = mrun[h : h + 1, :]
                best = jnp.maximum(old, best)
            weights = jnp.exp2((score - best) * EXP2_SCALE).astype(BF16)
            part = nn(vt[h, :, 0:keys], weights)
            if not masked:
                part += acc[h] * jnp.exp2((old - best) * EXP2_SCALE)
            acc[h] = part
            mrun[h : h + 1, :] = best

    own_to_partner.wait_recv()
    attend([(y, x)], masked=True)

    def place(b):
        yy = (y + pick(b, [a[0] for a in AWAY]) + 4) % 4
        xx = (x + pick(b, [a[1] for a in AWAY]) + 4) % 4
        return yy, xx

    def pass_on(b):
        yy, xx = place(b)
        for copy in other_slices(b, yy, xx):
            copy.wait_recv()
        to_partner(b, yy, xx).start()

    for copy in ends_x:
        copy.wait_recv()
    for h in range(NH):
        cols = slice(h * HD, (h + 1) * HD)
        to_end = sum(jnp.where(x < k, mx[k, h : h + 1, :], 0.0) for k in (1, 2, 3))
        faded = (endk[:, cols].astype(F32) * jnp.exp(to_end)).astype(BF16)
        for i in range(4):
            part = nn(tokt[i * 512 : (i + 1) * 512, :], faded).astype(BF16)
            for k in range(4):
                gw[h, i, k] = part[k * 128 : (k + 1) * 128, :]
    row_gw = [
        [
            remote(gw.at[h, :, (x + d) % 4], gwin.at[h, d - 1], gw_s.at[3 * h + d - 1], gw_r.at[3 * h + d - 1], x_peer(d))
            for d in (2, 1, 3)
        ]
        for h in range(NH)
    ]
    arrive(1)
    for copy in fwd_x:
        copy.start()
    pass_on(0)
    pass_on(1)
    for copy in rest_y:
        copy.start()

    def block_step(i, carry):
        @pl.when(i == LEVEL_STEP)
        def _():
            arrive(3)
            forward_row()

        for h, step in ((0, 3), (1, 4)):

            @pl.when(i == step)
            def _():
                for copy in row_gw[h]:
                    copy.start()

        ahead = jnp.logical_or(i == 0, i >= 3)

        @pl.when(jnp.logical_and(i < 7, ahead))
        def _():
            pass_on(2 * i + 2)

        @pl.when(jnp.logical_and(i < 6, ahead))
        def _():
            pass_on(2 * i + 3)

        @pl.when(i == 0)
        def _():
            for copy in rest_x:
                copy.start()

        @pl.when(i == 2)
        def _():
            for b, copies in ((6, rest_y), (7, rest_x)):
                for copy in copies:
                    copy.wait_recv()
                to_partner(b, *away(b)).start()

        y1, x1 = place(2 * i)
        to_partner(2 * i, y1, x1).wait_recv()
        y2, x2 = place(2 * i + 1)

        @pl.when(i < 7)
        def _():
            to_partner(2 * i + 1, y2, x2).wait_recv()

        need_1 = y1 * 4 + x1 < s
        need_2 = jnp.logical_and(y2 * 4 + x2 < s, i < 7)

        @pl.when(jnp.logical_and(need_1, need_2))
        def _():
            attend([(y1, x1), (y2, x2)])

        @pl.when(need_1 != need_2)
        def _():
            attend([(jnp.where(need_1, y1, y2), jnp.where(need_1, x1, x2))])

        @pl.when(i == 1)
        def _():
            arrive(2)
            pass_on(4)
            pass_on(5)

        return carry

    lax.fori_loop(0, 8, block_step, 0)

    for copy in fwd_y:
        copy.wait_recv()
    for h in range(NH):
        cols = slice(h * HD, (h + 1) * HD)
        inside_y = stage(sy, my, y, rise, h)[0]
        prefix = (held[cols, :] + jnp.exp(heldlog[h : h + 1, :]) * inside_y).astype(BF16)
        sout[:, cols] = sout[:, cols] + nn(startq[:, cols], prefix)

    def head_sends(buf, first, peer_of, slot, h):
        ref = buf.at[slot, h * HD : (h + 1) * HD, :]
        at = [first + 3 * h + d - 1 for d in (2, 1, 3)]
        return [remote(ref, ref, st_s.at[k], st_r.at[k], peer_of(d)) for k, d in zip(at, (2, 1, 3))]

    back_x = [head_sends(bx, 12, x_peer, x, h) for h in range(NH)]
    back_y = [head_sends(by, 18, y_peer, y, h) for h in range(NH)]
    squares = jnp.zeros((8, HD), F32)
    inv = 1.0 / math.sqrt(ALL_TOKENS)
    for h in range(NH):
        cols = slice(h * HD, (h + 1) * HD)
        teacher = jnp.transpose(acc[h, 0:HD, :] / acc[h, HD : HD + 1, :]).astype(BF16)
        tout_ref[:, cols] = teacher
        mismatch = sout[:, cols] - teacher.astype(F32)
        squares += jnp.sum((mismatch * mismatch).reshape(T // 8, 8, HD), axis=0)
        vg[:, cols] = (mismatch * inv).astype(BF16)
        bx[x, cols, :] = tn(startq[:, cols], vg[:, cols]).astype(BF16)
        for copy in back_x[h]:
            copy.start()
    lx[x] = squares
    ls = (ls_s, ls_r)
    loss_x = row_sends(lx, ls, 0, x_peer, x)
    for copy in loss_x:
        copy.start()
    for h in range(NH):
        cols = slice(h * HD, (h + 1) * HD)
        sout[:, cols] = tn(mix[h], vg[:, cols])

    row_inside = []
    for h in range(NH):
        for copy in back_x[h]:
            copy.wait_recv()
        inside, inside_log, running, _ = stage(bx, mx, x, fall, h)
        row_inside.append(inside.astype(BF16))
        by[y, h * HD : (h + 1) * HD, :] = running.astype(BF16)
        for copy in back_y[h]:
            copy.start()
    for copy in loss_x:
        copy.wait_recv()
    ly[y] = lx[0] + lx[1] + lx[2] + lx[3]
    loss_y = row_sends(ly, ls, 3, y_peer, y)
    for copy in loss_y:
        copy.start()

    def value_gradient(h):
        cols = slice(h * HD, (h + 1) * HD)
        vg[:, cols] = (sout[:, cols] + nn(endk[:, cols], row_inside[h])).astype(BF16)

    def from_later_rows(h):
        for copy in back_y[h]:
            copy.wait_recv()
        return nn(hrow[h], stage(by, my, y, fall, h)[0].astype(BF16))

    def weight_gradient(h):
        values = vg[:, h * HD : (h + 1) * HD]
        for i in range(4):
            part = nn(tokt[i * 512 : (i + 1) * 512, :], values).astype(BF16)
            for k in range(4):
                pw[h, i, k] = part[k * 128 : (k + 1) * 128, :]

    rs_x1 = [
        remote(pw.at[0, :, (x + d) % 4], r1in.at[0, d - 1], rs_s.at[d - 1], rs_r.at[d - 1], x_peer(d))
        for d in (2, 1, 3)
    ]
    rs_y1 = [
        remote(
            pw.at[1, (y + d) % 4, :, NA:, :],
            r1in.at[1, d - 1, :, NA:, :],
            rs_s.at[d + 2],
            rs_r.at[d + 2],
            y_peer(d),
        )
        for d in (1, 3, 2)
    ]
    rs_a1 = [
        remote(pw.at[1, :, (x + d) % 4, 0:NA, :], a1in.at[d - 1], rs_s.at[d + 14], rs_r.at[d + 14], x_peer(d))
        for d in (2, 1, 3)
    ]
    value_gradient(0)
    value_gradient(1)
    weight_gradient(1)
    for copy in rs_y1 + rs_a1:
        copy.start()
    weight_gradient(0)
    for copy in rs_x1:
        copy.start()
    for h in range(NH):
        for copy in row_gw[h]:
            copy.wait_recv()
        for k in range(4):
            total = gw[h, k, x].astype(F32) + sum(gwin[h, d, k].astype(F32) for d in range(3))
            hrow[h, k * 128 : (k + 1) * 128, :] = total.astype(BF16)
    later = from_later_rows(0)
    later_1 = from_later_rows(1)
    for k in range(4):
        lown[k] = later_1[k * 128 + NA : (k + 1) * 128, :].astype(BF16)
    rows_y = [
        remote(lown.at[(y + d) % 4], lin.at[d - 1], rs_s.at[d + 11], rs_r.at[d + 11], y_peer(d)) for d in (2, 1, 3)
    ]
    for copy in rows_y:
        copy.start()
    for copy in loss_y:
        copy.wait_recv()
    lz[z] = ly[0] + ly[1] + ly[2] + ly[3]
    loss_z = row_sends(lz, ls, 6, z_peer, z)
    for copy in loss_z:
        copy.start()

    for copy in rs_x1:
        copy.wait_recv()
    mine = [pw[0, k, x].astype(F32) for k in range(4)]
    for k in range(4):
        total = mine[k] + later[k * 128 : (k + 1) * 128, :]
        r1own[0, k] = (total + sum(r1in[0, d, k].astype(F32) for d in range(3))).astype(BF16)
    rs_y2 = [
        remote(r1own.at[0, (y + d) % 4], r2in.at[0, d - 1], rs_s.at[d + 5], rs_r.at[d + 5], y_peer(d))
        for d in (2, 1, 3)
    ]
    for copy in rs_y2:
        copy.start()
    for copy in rs_a1:
        copy.wait_recv()
    for k in range(4):
        total = pw[1, k, x, 0:NA, :].astype(F32) + later_1[k * 128 : k * 128 + NA, :]
        a1own[k] = (total + sum(a1in[d, k].astype(F32) for d in range(3))).astype(BF16)
    rs_a2 = [
        remote(a1own.at[(y + d) % 4], a2in.at[d - 1], rs_s.at[d + 17], rs_r.at[d + 17], y_peer(d)) for d in (2, 1, 3)
    ]
    for copy in rs_a2:
        copy.start()
    for copy in rs_y1:
        copy.wait_recv()
    mine = [pw[1, y, k, NA:, :].astype(F32) for k in range(4)]
    for k in range(4):
        total = mine[k] + sum(r1in[1, d, k, NA:, :].astype(F32) for d in range(3))
        r1own[1, k, NA:, :] = total.astype(BF16)
    rs_x2 = [
        remote(
            r1own.at[1, (x + d) % 4, NA:, :],
            r2in.at[1, d - 1, NA:, :],
            rs_s.at[d + 8],
            rs_r.at[d + 8],
            x_peer(d),
        )
        for d in (2, 1, 3)
    ]
    for copy in rs_x2:
        copy.start()

    for copy in loss_z:
        copy.wait_recv()
    lc[c] = lz[0] + lz[1] + lz[2] + lz[3]
    loss_c = remote(lc.at[c], lc.at[c], ls_s.at[9], ls_r.at[9], partner)
    loss_c.start()
    loss_c.wait_recv()
    loss_ref[0, 0] = jnp.sum(lc[0] + lc[1]) / (2.0 * ALL_TOKENS * ALL_HEADS * HD)

    for copy in rs_y2:
        copy.wait_recv()
    wg_ref[:, 0:HD] = r1own[0, y].astype(F32) + sum(r2in[0, d].astype(F32) for d in range(3))
    for copy in rows_y:
        copy.wait_recv()
    late = lown[y].astype(F32) + sum(lin[d].astype(F32) for d in range(3))
    for copy in rs_x2:
        copy.wait_recv()
    partial = r1own[1, x, NA:, :].astype(F32) + sum(r2in[1, d, NA:, :].astype(F32) for d in range(3))
    wg_ref[NA:, HD:W] = late + partial
    for copy in rs_a2:
        copy.wait_recv()
    wg_ref[0:NA, HD:W] = a1own[y].astype(F32) + sum(a2in[d].astype(F32) for d in range(3))

    sent = [to_pair] + to_z + fwd_x + fwd_y + sum(back_x + back_y, [])
    sent += loss_x + loss_y + loss_z + [loss_c] + rs_x1 + rs_y1 + rs_y2 + rs_x2
    sent += rs_a1 + rs_a2 + ends_x + sum(row_gw, []) + rows_y
    for level in levels:
        sent += level
    for b in range(15):
        sent += [to_partner(b, *away(b))]
    for blocks in LEVEL_OVER_Z:
        for b in blocks:
            sent += other_slices(b, *away(b))
    sent += rest_x + rest_y
    sent.append(own_to_partner)
    for copy in sent:
        copy.wait_send()


def finish(teacher_ref, wgrad_ref, teacher_out, wgrad_out, sem):
    copies = [
        pltpu.make_async_copy(teacher_ref, teacher_out, sem.at[0]),
        pltpu.make_async_copy(wgrad_ref, wgrad_out, sem.at[1]),
    ]
    for copy in copies:
        copy.start()
    for copy in copies:
        copy.wait()


def per_device(tokens, w_latent, w_query, w_key_up, w_value_up, w_stu_query, w_stu_key, w_stu_value, forget):
    dma = pltpu.SemaphoreType.DMA
    scratch = [
        pltpu.VMEM((T, D), BF16),
        pltpu.VMEM((D, T), BF16),
        pltpu.VMEM((HD, D), BF16),
        pltpu.VMEM((4, D, W), BF16),
        pltpu.VMEM((LAT, W), BF16),
        pltpu.VMEM((LAT, W), BF16),
        pltpu.VMEM((W, LAT), BF16),
        pltpu.VMEM((NH, T), F32),
        pltpu.VMEM((4, 4, 4, T, HD), BF16),
        pltpu.VMEM((T, HD), BF16),
        pltpu.VMEM((HALF, HD), BF16),
        pltpu.VMEM((HALF, HD), BF16),
        pltpu.VMEM((2 * T, W), BF16),
        pltpu.VMEM((NH, HD + ONES, 2 * T), BF16),
        pltpu.VMEM((T, W), BF16),
        pltpu.VMEM((NH, HD + ONES, T), F32),
        pltpu.VMEM((8, T), F32),
        pltpu.VMEM((T, W), BF16),
        pltpu.VMEM((T, W), BF16),
        pltpu.VMEM((T, W), BF16),
        pltpu.VMEM((NH, T, HD), F32),
        pltpu.VMEM((8, T), F32),
        pltpu.VMEM((NH, T, T), BF16),
        pltpu.VMEM((T, W), F32),
        pltpu.VMEM((T, W), BF16),
        pltpu.VMEM((T, W), BF16),
        pltpu.VMEM((T, W), BF16),
        pltpu.VMEM((W, HD), F32),
        pltpu.VMEM((8, HD), F32),
        pltpu.VMEM((4, W, HD), BF16),
        pltpu.VMEM((4, W, HD), BF16),
        pltpu.VMEM((4, 8, HD), F32),
        pltpu.VMEM((4, 8, HD), F32),
        pltpu.VMEM((4, W, HD), BF16),
        pltpu.VMEM((4, W, HD), BF16),
        pltpu.VMEM((4, 8, HD), F32),
        pltpu.VMEM((4, 8, HD), F32),
        pltpu.VMEM((4, 8, HD), F32),
        pltpu.VMEM((2, 8, HD), F32),
        pltpu.VMEM((NH, 4, 4, 128, HD), BF16),
        pltpu.VMEM((NH, 3, 4, 128, HD), BF16),
        pltpu.VMEM((NH, 4, 128, HD), BF16),
        pltpu.VMEM((NH, 3, 128, HD), BF16),
        pltpu.VMEM((NH, 4, 4, 128, HD), BF16),
        pltpu.VMEM((NH, 3, 4, 128, HD), BF16),
        pltpu.VMEM((NH, 512, HD), BF16),
        pltpu.VMEM((4, 128 - NA, HD), BF16),
        pltpu.VMEM((3, 128 - NA, HD), BF16),
        pltpu.VMEM((3, 4, NA, HD), BF16),
        pltpu.VMEM((4, NA, HD), BF16),
        pltpu.VMEM((3, NA, HD), BF16),
        dma((15,)),
        dma,
        dma,
        dma((3,)),
        dma((3,)),
        dma((44,)),
        dma((44,)),
        dma((30,)),
        dma((30,)),
        dma((16,)),
        dma((16,)),
        dma((24,)),
        dma((24,)),
        dma((21,)),
        dma((21,)),
        dma((10,)),
        dma((10,)),
        dma((6,)),
        dma((6,)),
    ]
    anywhere = pl.BlockSpec(memory_space=pl.ANY)
    teacher, loss, wgrad = pl.pallas_call(
        kernel,
        out_shape=(
            pltpu.VMEM((T, W), BF16),
            jax.ShapeDtypeStruct((1, 1), F32),
            pltpu.VMEM((128, W), F32),
        ),
        in_specs=[anywhere] * 9,
        out_specs=(
            pl.BlockSpec(memory_space=pltpu.VMEM),
            pl.BlockSpec(memory_space=pltpu.SMEM),
            pl.BlockSpec(memory_space=pltpu.VMEM),
        ),
        scratch_shapes=scratch,
        compiler_params=pltpu.CompilerParams(
            collective_id=0, has_side_effects=True, vmem_limit_bytes=60 * 1024 * 1024
        ),
    )(
        tokens, w_latent.T, w_query, w_key_up, w_value_up, w_stu_query, w_stu_key, w_stu_value, forget.T
    )
    teacher, wgrad = pl.pallas_call(
        finish,
        out_shape=(jax.ShapeDtypeStruct((T, W), BF16), jax.ShapeDtypeStruct((128, W), F32)),
        in_specs=[pl.BlockSpec(memory_space=pltpu.VMEM)] * 2,
        out_specs=(anywhere, anywhere),
        scratch_shapes=[dma((2,))],
        compiler_params=pltpu.CompilerParams(vmem_limit_bytes=4 * 1024 * 1024),
    )(teacher, wgrad)
    return teacher, loss[0, 0], wgrad


def solution(mesh):
    return jax.shard_map(
        per_device,
        mesh=mesh,
        in_specs=(
            P("seq", None),
            P(None, "tensor"),
            P(None, "tensor"),
            P(None, "tensor"),
            P(None, "tensor"),
            P(None, "tensor"),
            P(None, "tensor"),
            P(None, "tensor"),
            P("seq", "tensor"),
        ),
        out_specs=(P("seq", "tensor"), P(), P("seq", "tensor")),
        check_vma=False,
    )
```
